256 devices in a mesh: ang: 32 (over y, z_hi, x), slab: 8 (over z_lo, core).
Axes of the slice: x: 4, y: 4, z: 8 (z_hi: 2, z_lo: 4; z = z_hi * 4 + z_lo), core: 2. Of those that a mesh axis runs over, the one named last changes fastest.
Arguments:
- updates: float32 [128, 2, 1024, 512], P('ang', None, 'slab'), may hold values from -6 to 6
- interp_tiles: bfloat16 [128, 32, 256, 128], P('ang'), may hold values from -0.25 to 0.25
- band_start: int32 [128, 32], P('ang'), may hold values from 0 to 2
- angle_id: int32 [128], P('ang'), may hold values from 0 to 127, each once
- angle_weight: float32 [128], replicated, may hold values from 0.05 to 0.5
- volume: float32 [4096, 2, 1024], P('ang', None, 'slab'), may hold values from -6 to 6
Outputs:
- volume_next: float32 [4096, 2, 1024], P('ang', None, 'slab')
- projection: float32 [128, 2, 1024, 512], P('ang', None, 'slab')
The draws below stay inside these ranges and needn't reach their ends.
Inputs may be any that keep to these rules, and one draw needn't show every extreme that they name: Tile j of angle slot a reads detector columns 128 * band_start[a, j] up to 256 further. `angle_id`: each measured angle stands in exactly one slot.
All inputs are finite; a program needn't handle non-finite values.
Results may differ from the reference program's by a relative error of at most 0.0062.
Values may be sent and summed in bfloat16 or wider, within the bound.
A program may use at most 128 MiB of HBM per device.

```python
import math
import jax
import jax.numpy as jnp
from jax import lax

S = 512
BLOCK = 128
BAND = 256
XW = 8
ANGLES = 128
Z = 1024
CELLS = 4096
TILES = 32


def with_ends(entries, own_key, low, largest):
    index_at = [jax.random.randint(jax.random.fold_in(own_key, axis), (), 0, length) for axis, length in enumerate(entries.shape)]
    longest = entries.shape.index(max(entries.shape))
    beside = index_at[:longest] + [(index_at[longest] + 1) % entries.shape[longest]] + index_at[longest + 1:]
    return entries.at[tuple(index_at)].set(low).at[tuple(beside)].set(largest)


def strengthened(values, stream_key, source, target, parts, factor):
    owner, partner = [(jnp.arange(values.shape[dim]) // (values.shape[dim] // parts)).reshape([-1 if axis == dim else 1 for axis in range(values.ndim)]) for dim in (source, target)]
    chosen = jax.random.permutation(stream_key, parts)[partner]
    strong = (owner == chosen) | (owner == (partner + parts // 2) % parts)
    return jnp.where(strong, factor * values, values)


def steps_of(rng, shape, pieces, smallest, largest):
    factor_of, own = 1.0, jax.random.fold_in(rng, 6)
    for position, blocks in pieces:
        steps = jnp.exp(jax.random.uniform(jax.random.fold_in(own, position), (blocks,), jnp.float32, smallest / len(pieces), largest / len(pieces)))
        factor_of = factor_of * jnp.repeat(steps, shape[position] // blocks).reshape([-1 if axis == position else 1 for axis in range(len(shape))])
    return factor_of


def gaussian(key, extent, spread, most, pieces=(), kind=jnp.bfloat16):
    drawn = spread * jax.random.normal(key, extent, jnp.float32)
    if pieces:
        drawn = drawn * steps_of(key, extent, pieces, -0.22, 0.18)
    return jnp.clip(drawn, -most, most).astype(kind)


def noise_with(rng, extent, scale, bound, pieces, heavy, held_as=jnp.bfloat16):
    values = scale * jax.random.normal(rng, extent, jnp.float32)
    if pieces:
        values = values * steps_of(rng, extent, pieces, -0.22, 0.18)
    return jnp.clip(strengthened(values, jax.random.fold_in(rng, 3), *heavy), -bound, bound).astype(held_as)


def setup_inputs(seed: int = 0) -> dict:
    streams_of = jax.random.split(jax.random.key(seed), 7)
    updates = gaussian(streams_of[0], (ANGLES, 2, Z, S), 1.0, 6.0, ((0, 32), (2, 8)), jnp.float32)
    interp_tiles = noise_with(streams_of[1], (ANGLES, TILES, BAND, BLOCK), (BAND * XW) ** -0.5, 0.25, ((0, 32),), (0, 1, 32, 2.75))
    band_start = with_ends(jax.random.randint(streams_of[2], (ANGLES, TILES), 0, S // BLOCK - 1), jax.random.fold_in(streams_of[2], 1), 0, (S // BLOCK - 1) - 1).astype(jnp.int32)
    angle_id = jax.random.permutation(streams_of[3], ANGLES).astype(jnp.int32)
    angle_weight = jnp.clip(jnp.exp(jax.random.uniform(streams_of[4], (ANGLES,), jnp.float32, math.log(0.05), math.log(0.5))), 0.05, 0.5)
    volume = gaussian(streams_of[5], (CELLS, 2, Z), 1.0, 6.0, ((0, 32), (2, 8)), jnp.float32)
    return dict(updates=updates, interp_tiles=interp_tiles, band_start=band_start, angle_id=angle_id, angle_weight=angle_weight, volume=volume)


SMOOTHING = 0.25


def clamp_absorption(field):
    channel = jnp.arange(2, dtype=jnp.int32)[None, :, None]
    return jnp.where(channel == 1, jnp.maximum(field, 0.0), field)


def band_windows(row_block, starts):
    def take_window(first_block):
        return lax.dynamic_slice_in_dim(row_block, first_block * BLOCK, BAND, axis=1)
    return jax.vmap(take_window)(starts)


def place_bands(images, starts):
    positions = jnp.arange(S // BLOCK - 1, dtype=jnp.int32)
    onehot = (starts[:, None] == positions[None, :]).astype(jnp.float32)
    grouped = jnp.einsum('jk,jrq->krq', onehot, images, precision=lax.Precision.HIGHEST)
    result = jnp.zeros((images.shape[1], S), jnp.float32)
    for offset_index in range(S // BLOCK - 1):
        result = result + jnp.pad(grouped[offset_index], ((0, 0), (BLOCK * offset_index, S - BLOCK * offset_index - BAND)))
    return result


def reference(updates, interp_tiles, band_start, angle_id, angle_weight, volume):
    row_count = 2 * Z
    matches = angle_id[:, None] == jnp.arange(ANGLES, dtype=jnp.int32)[None, :]
    chosen = jnp.sum(jnp.where(matches, angle_weight[None, :], 0.0), axis=1)
    scaled = (chosen[:, None, None, None] * updates).astype(jnp.bfloat16).reshape(ANGLES, row_count, S)

    def back_step(summed, packed):
        row_block, tile_set, starts = packed
        windows = band_windows(row_block, starts).astype(jnp.float32)
        term = jnp.einsum('jrq,jqp->jpr', windows, tile_set.astype(jnp.float32))
        return summed + term, 0

    initial = jnp.zeros((TILES, BLOCK, row_count), jnp.float32)
    summed = lax.scan(back_step, initial, (scaled, interp_tiles, band_start))[0]
    partial_sum = summed.reshape(CELLS, 2, Z)
    padded = jnp.pad(volume, ((0, 0), (0, 0), (1, 1)))
    smooth = volume - SMOOTHING * (2.0 * volume - padded[:, :, :-2] - padded[:, :, 2:])
    volume_next = clamp_absorption(smooth + partial_sum)
    lowered = lax.optimization_barrier(volume_next.astype(jnp.bfloat16))
    lowered = lowered.astype(jnp.float32).reshape(TILES, BLOCK, row_count)

    def forward_one(packed):
        tile_set, starts = packed
        images = jnp.einsum('jpr,jqp->jrq', lowered, tile_set.astype(jnp.float32))
        return place_bands(images, starts)

    projection = lax.map(forward_one, (interp_tiles, band_start))
    return volume_next, projection.reshape(ANGLES, 2, Z, S)
```

```python
import functools

import jax
import jax.numpy as jnp
from jax import lax
from jax.experimental import pallas as pl
from jax.experimental.pallas import tpu as pltpu
from jax.sharding import PartitionSpec as P

SMOOTHING = 0.25
MESH = pl.DeviceIdType.MESH
BF = jnp.bfloat16
F32 = jnp.float32
NX, NY, NH = 4, 4, 2
SLABS = 8
GROUP_ORDER = (2, 1, 3, 0)


def device(x, y, h, s):
    return (y * (NH * NX) + h * NX + x, s)


def wrapped(v, n):
    return lax.rem(v + n, n)


def exchange_kernel(
    band_ref,
    id_ref,
    weight_ref,
    upd_hbm,
    tiles_hbm,
    vol_ref,
    vnext_ref,
    gath,
    upd,
    tiles,
    scaled,
    part,
    vt,
    halo,
    smooth,
    smooth_in,
    r1,
    s2,
    r2,
    keep,
    zs,
    rz,
    upd_sem,
    tile_sem,
    halo_ss,
    halo_rs,
    sm_ss,
    sm_rs,
    ss1,
    rs1,
    ss2,
    rs2,
    zss,
    zrs,
    ass1,
    ars1,
    ass2,
    ars2,
):
    me = lax.axis_index("ang")
    s = lax.axis_index("slab")
    x = lax.rem(me, NX)
    h = lax.rem(me // NX, NH)
    y = me // (NX * NH)
    sl = wrapped(s - 1, SLABS)
    sr = wrapped(s + 1, SLABS)
    xs = [wrapped(x + d, NX) for d in range(4)]
    ys = [wrapped(y + d, NY) for d in range(4)]

    barrier = pltpu.get_barrier_semaphore()
    peers = (
        [device(xs[d], y, h, s) for d in (1, 2, 3)]
        + [device(x, ys[d], h, s) for d in (1, 2, 3)]
        + [device(x, y, 1 - h, s), device(x, y, h, sl), device(x, y, h, sr)]
    )
    for peer in peers:
        pl.semaphore_signal(barrier, inc=1, device_id=peer, device_id_type=MESH)

    upd_copies = [pltpu.make_async_copy(upd_hbm.at[a], upd.at[a], upd_sem.at[a]) for a in range(4)]
    for copy in upd_copies:
        copy.start()

    def tile_copy(ty, th, tx):
        j = ty * (NH * NX) + th * NX + tx
        return pltpu.make_async_copy(tiles_hbm.at[:, j], tiles.at[j], tile_sem.at[j])

    for d in GROUP_ORDER:

        def start_tiles(i, carry, d=d):
            tile_copy(i, 0, xs[d]).start()
            tile_copy(ys[d], 1, i).start()
            return carry

        lax.fori_loop(0, 4, start_tiles, 0)

    for c in range(2):
        vt[c] = vol_ref[:, c, :].T
    lanes = lax.broadcasted_iota(jnp.int32, (1, 128), 1)
    for a in range(4):
        matched = jnp.where(lanes == id_ref[a], weight_ref[...], 0.0)
        chosen = jnp.sum(matched, axis=1, keepdims=True)
        upd_copies[a].wait()
        value = (chosen * upd[a]).astype(BF)
        for k in range(3):
            scaled[3 * a + k] = value[:, 128 * k : 128 * k + 256]

    def one_tile(ty, th, tx):
        j = ty * (NH * NX) + th * NX + tx
        tile_copy(ty, th, tx).wait()
        windows = [scaled[3 * a + band_ref[a, j]] for a in range(4)]
        total = jnp.dot(
            jnp.concatenate(windows, axis=1),
            tiles[j].reshape(4 * 256, 128),
            preferred_element_type=F32,
        )
        part[ty, th, tx] = total.astype(BF)

    def remote(src, dst, send, recv, where):
        return pltpu.make_async_remote_copy(
            src_ref=src,
            dst_ref=dst,
            send_sem=send,
            recv_sem=recv,
            device_id=where,
            device_id_type=MESH,
        )

    def rows(c):
        return slice(c * 128, c * 128 + 128)

    def first(path, c, d):
        if path == 0:
            src, where = part.at[:, 0, xs[d], rows(c), :], device(xs[d], y, h, s)
        else:
            src, where = part.at[ys[d], 1, :, rows(c), :], device(x, ys[d], h, s)
        return remote(
            src, r1.at[path, c, d - 1], ss1.at[path, c, d - 1], rs1.at[path, c, d - 1], where
        )

    def second(path, c, d):
        where = device(x, ys[d], h, s) if path == 0 else device(xs[d], y, h, s)
        return remote(
            s2.at[path, c, d - 1],
            r2.at[path, c, d - 1],
            ss2.at[path, c, d - 1],
            rs2.at[path, c, d - 1],
            where,
        )

    def across(path, c):
        return remote(
            zs.at[path, c], rz.at[path, c], zss.at[path, c], zrs.at[path, c], device(x, y, 1 - h, s)
        )

    def gather1(path, c, d):
        where = device(x, ys[d], h, s) if path == 0 else device(xs[d], y, h, s)
        ref = gath.at[y, path, x, :, rows(c)]
        return remote(ref, ref, ass1.at[path, c, d - 1], ars1.at[path, c, d - 1], where)

    def gather2(path, c, d):
        if path == 0:
            ref, where = gath.at[:, 0, x, :, rows(c)], device(xs[d], y, h, s)
        else:
            ref, where = gath.at[y, 1, :, :, rows(c)], device(x, ys[d], h, s)
        return remote(ref, ref, ass2.at[path, c, d - 1], ars2.at[path, c, d - 1], where)

    def halo_copy(c, side):
        if side == 0:
            src, where = vt.at[c, 120:128, :], device(x, y, h, sr)
        else:
            src, where = vt.at[c, 0:8, :], device(x, y, h, sl)
        return remote(src, halo.at[c, side], halo_ss.at[c, side], halo_rs.at[c, side], where)

    smooth_copy = remote(smooth, smooth_in, sm_ss, sm_rs, device(x, y, 1 - h, s))

    for position, d in enumerate(GROUP_ORDER):

        def group(i, carry, d=d):
            for u in range(2):
                one_tile(2 * i + u, 0, xs[d])
                one_tile(ys[d], 1, 2 * i + u)
            return carry

        lax.fori_loop(0, 2, group, 0)
        if position == 0:
            pl.semaphore_wait(barrier, len(peers))
            for c in range(2):
                halo_copy(c, 0).start()
                halo_copy(c, 1).start()
        if d:
            for c in range(2):
                first(0, c, d).start()
                first(1, c, d).start()
        if position == 1:
            for c in range(2):
                halo_copy(c, 0).wait_recv()
                halo_copy(c, 1).wait_recv()
                mid = vt[c]
                row = lax.broadcasted_iota(jnp.int32, (128, 128), 0)
                low = jnp.where(s > 0, halo[c, 0, 7:8, :], 0.0)
                high = jnp.where(s < SLABS - 1, halo[c, 1, 0:1, :], 0.0)
                before = jnp.where(row == 0, low, pltpu.roll(mid, 1, 0))
                after = jnp.where(row == 127, high, pltpu.roll(mid, 127, 0))
                smooth[c] = mid - SMOOTHING * (2.0 * mid - before - after)
            smooth_copy.start()

    for c in range(2):
        for path in range(2):
            for d in (1, 2, 3):
                first(path, c, d).wait_recv()
            for d in (2, 1, 3, 0):
                at = ys[d] if path == 0 else xs[d]
                own = part[at, 0, x, rows(c), :] if path == 0 else part[y, 1, at, rows(c), :]
                total = own.astype(F32)
                for k in range(3):
                    total = total + r1[path, c, k, at].astype(F32)
                if d:
                    s2[path, c, d - 1] = total.astype(BF)
                    second(path, c, d).start()
                else:
                    keep[path, c] = total

    for c in range(2):
        for path in range(2):
            for d in (1, 2, 3):
                second(path, c, d).wait_recv()
            total = keep[path, c]
            for k in range(3):
                total = total + r2[path, c, k].astype(F32)
            keep[path, c] = total
            zs[path, c] = total.astype(BF)
            across(path, c).start()

    smooth_copy.wait_recv()
    for c in range(2):
        fields = []
        for path in range(2):
            across(path, c).wait_recv()
            base = jnp.where(h == path, smooth[c], smooth_in[c])
            field = base + (keep[path, c] + rz[path, c].astype(F32))
            if c == 1:
                field = jnp.maximum(field, 0.0)
            field = field.T
            fields.append(field)
            gath[y, path, x, :, rows(c)] = field.astype(BF)
            for d in (2, 1, 3):
                gather1(path, c, d).start()
        vnext_ref[:, c, :] = jnp.where(h == 0, fields[0], fields[1])

    for c in range(2):
        for path in range(2):
            for d in (1, 2, 3):
                gather1(path, c, d).wait_recv()
            for d in (2, 1, 3):
                gather2(path, c, d).start()

    for c in range(2):
        for path in range(2):
            for d in (1, 2, 3):
                gather2(path, c, d).wait_recv()

    smooth_copy.wait_send()
    for c in range(2):
        halo_copy(c, 0).wait_send()
        halo_copy(c, 1).wait_send()
        for path in range(2):
            across(path, c).wait_send()
            for d in (1, 2, 3):
                first(path, c, d).wait_send()
                second(path, c, d).wait_send()
                gather1(path, c, d).wait_send()
                gather2(path, c, d).wait_send()


def placed_rows(tile, start):
    low, high = tile[:128], tile[128:]
    zero = jnp.zeros_like(low)
    return jnp.concatenate(
        [
            jnp.where(start == 0, low, zero),
            jnp.where(start == 0, high, jnp.where(start == 1, low, zero)),
            jnp.where(start == 1, high, jnp.where(start == 2, low, zero)),
            jnp.where(start == 2, high, zero),
        ],
        axis=0,
    )


def project_kernel(band_ref, tiles_ref, gath_ref, out_ref, acc):
    a = pl.program_id(0)

    def group(g, carry):
        left = jnp.concatenate(
            [placed_rows(tiles_ref[0, g * 8 + u], band_ref[a, g * 8 + u]) for u in range(8)], axis=1
        )
        right = gath_ref[pl.ds(g * 8, 8)].reshape(8 * 128, 256)
        term = jnp.dot(left, right, preferred_element_type=F32)
        acc[...] = jnp.where(g == 0, term, acc[...] + term)
        return carry

    lax.fori_loop(0, 4, group, 0)
    out_ref[0] = acc[...].T


def shards(updates, interp_tiles, band_start, angle_id, angle_weight, volume):
    smem = pl.BlockSpec(memory_space=pltpu.SMEM)
    vmem = pl.BlockSpec(memory_space=pltpu.VMEM)
    hbm = pl.BlockSpec(memory_space=pl.ANY)
    dma = pltpu.SemaphoreType.DMA
    vnext, gath = pl.pallas_call(
        exchange_kernel,
        out_shape=(
            jax.ShapeDtypeStruct((128, 2, 128), F32),
            jax.ShapeDtypeStruct((4, 2, 4, 128, 256), BF),
        ),
        in_specs=[smem, smem, vmem, hbm, hbm, vmem],
        out_specs=(vmem, vmem),
        scratch_shapes=[
            pltpu.VMEM((4, 256, 512), F32),
            pltpu.VMEM((32, 4, 256, 128), BF),
            pltpu.VMEM((12, 256, 256), BF),
            pltpu.VMEM((4, 2, 4, 256, 128), BF),
            pltpu.VMEM((2, 128, 128), F32),
            pltpu.VMEM((2, 2, 8, 128), F32),
            pltpu.VMEM((2, 128, 128), F32),
            pltpu.VMEM((2, 128, 128), F32),
            pltpu.VMEM((2, 2, 3, 4, 128, 128), BF),
            pltpu.VMEM((2, 2, 3, 128, 128), BF),
            pltpu.VMEM((2, 2, 3, 128, 128), BF),
            pltpu.VMEM((2, 2, 128, 128), F32),
            pltpu.VMEM((2, 2, 128, 128), BF),
            pltpu.VMEM((2, 2, 128, 128), BF),
            dma((4,)),
            dma((32,)),
            dma((2, 2)),
            dma((2, 2)),
            dma,
            dma,
            dma((2, 2, 3)),
            dma((2, 2, 3)),
            dma((2, 2, 3)),
            dma((2, 2, 3)),
            dma((2, 2)),
            dma((2, 2)),
            dma((2, 2, 3)),
            dma((2, 2, 3)),
            dma((2, 2, 3)),
            dma((2, 2, 3)),
        ],
        compiler_params=pltpu.CompilerParams(
            collective_id=0, has_side_effects=True, vmem_limit_bytes=44 * 2**20
        ),
        name="exchange",
    )(
        band_start,
        angle_id,
        angle_weight.reshape(1, 128),
        updates.reshape(4, 256, 512),
        interp_tiles,
        volume,
    )
    projection = pl.pallas_call(
        project_kernel,
        grid=(4,),
        out_shape=jax.ShapeDtypeStruct((4, 256, 512), F32),
        in_specs=[
            smem,
            pl.BlockSpec((1, 32, 256, 128), lambda a: (a, 0, 0, 0)),
            vmem,
        ],
        out_specs=pl.BlockSpec((1, 256, 512), lambda a: (a, 0, 0)),
        scratch_shapes=[pltpu.VMEM((512, 256), F32)],
        compiler_params=pltpu.CompilerParams(vmem_limit_bytes=32 * 2**20),
        name="project",
    )(band_start, interp_tiles, gath.reshape(32, 128, 256))
    return vnext, projection.reshape(4, 2, 128, 512)


def solution(mesh):
    placed = (
        P("ang", None, "slab", None),
        P("ang", None, None, None),
        P("ang", None),
        P("ang"),
        P(),
        P("ang", None, "slab"),
    )
    return jax.shard_map(
        shards,
        mesh=mesh,
        in_specs=placed,
        out_specs=(P("ang", None, "slab"), P("ang", None, "slab", None)),
        check_vma=False,
    )
```

```python
import jax
import jax.numpy as jnp
from jax import lax
from jax.experimental import pallas as pl
from jax.experimental.pallas import tpu as pltpu
from jax.sharding import PartitionSpec as P

SMOOTHING = 0.25
MESH = pl.DeviceIdType.MESH
BF = jnp.bfloat16
F32 = jnp.float32
NX, NY, NH = 4, 4, 2
SLABS = 8
ANG = 4
FAR = (2, 1, 3)


def device(x, y, h, s):
    return (y * (NH * NX) + h * NX + x, s)


def wrapped(v, n):
    return lax.rem(v + n, n)


def placed_rows(tile, start):
    low, high = tile[:128], tile[128:]
    zero = jnp.zeros_like(low)
    return jnp.concatenate(
        [
            jnp.where(start == 0, low, zero),
            jnp.where(start == 0, high, jnp.where(start == 1, low, zero)),
            jnp.where(start == 1, high, jnp.where(start == 2, low, zero)),
            jnp.where(start == 2, high, zero),
        ],
        axis=0,
    )


def whole_kernel(
    band_hbm,
    id_hbm,
    weight_hbm,
    upd_hbm,
    tiles_hbm,
    vol_hbm,
    vnext_ref,
    out_ref,
    band_ref,
    id_ref,
    weight_ref,
    vol_ref,
    upd,
    tiles,
    scaled,
    part,
    vt,
    halo,
    smooth,
    smooth_in,
    r1,
    s2,
    r2,
    keep,
    zs,
    rz,
    gath,
    acc,
    in_sem,
    tile_sem,
    halo_ss,
    halo_rs,
    sm_ss,
    sm_rs,
    ss1,
    rs1,
    ss2,
    rs2,
    zss,
    zrs,
    ass1,
    ars1,
    ass2,
    ars2,
):
    me = lax.axis_index("ang")
    s = lax.axis_index("slab")
    x = lax.rem(me, NX)
    h = lax.rem(me // NX, NH)
    y = me // (NX * NH)
    sl = wrapped(s - 1, SLABS)
    sr = wrapped(s + 1, SLABS)
    xs = [wrapped(x + d, NX) for d in range(4)]
    ys = [wrapped(y + d, NY) for d in range(4)]

    barrier = pltpu.get_barrier_semaphore()
    peers = (
        [device(xs[d], y, h, s) for d in (1, 2, 3)]
        + [device(x, ys[d], h, s) for d in (1, 2, 3)]
        + [device(x, y, 1 - h, s), device(x, y, h, sl), device(x, y, h, sr)]
    )
    for peer in peers:
        pl.semaphore_signal(barrier, inc=1, device_id=peer, device_id_type=MESH)

    def tile_copy(ty, th, tx):
        j = ty * (NH * NX) + th * NX + tx
        return pltpu.make_async_copy(tiles_hbm.at[:, j], tiles.at[j], tile_sem.at[j])

    def start_tiles(d):
        def body(i, carry):
            tile_copy(i, 0, xs[d]).start()
            tile_copy(ys[d], 1, i).start()
            return carry

        lax.fori_loop(0, 4, body, 0)

    band_copy = pltpu.make_async_copy(band_hbm, band_ref, in_sem.at[0])
    id_copy = pltpu.make_async_copy(id_hbm, id_ref, in_sem.at[1])
    weight_copy = pltpu.make_async_copy(weight_hbm, weight_ref, in_sem.at[2])
    vol_copy = pltpu.make_async_copy(vol_hbm, vol_ref, in_sem.at[3])
    upd_copies = [pltpu.make_async_copy(upd_hbm.at[:, c], upd.at[c], in_sem.at[4 + c]) for c in (0, 1)]
    id_copy.start()
    weight_copy.start()
    upd_copies[0].start()
    band_copy.start()
    start_tiles(2)
    vol_copy.start()
    start_tiles(1)
    start_tiles(3)
    upd_copies[1].start()
    start_tiles(0)

    def rows(c):
        return slice(c * 128, c * 128 + 128)

    lanes = lax.broadcasted_iota(jnp.int32, (1, 128), 1)
    id_copy.wait()
    weight_copy.wait()
    chosen = [
        jnp.sum(jnp.where(lanes == id_ref[a], weight_ref[...], 0.0), axis=1, keepdims=True)
        for a in range(ANG)
    ]

    def scale(c):
        upd_copies[c].wait()
        for a in range(ANG):
            value = (chosen[a] * upd[c, a]).astype(BF)
            for k in range(3):
                scaled[c, 3 * a + k] = value[:, 128 * k : 128 * k + 256]

    def one_tile(c, ty, th, tx):
        j = ty * (NH * NX) + th * NX + tx
        if c == 0:
            tile_copy(ty, th, tx).wait()
        windows = [scaled[c, 3 * a + band_ref[a, j]] for a in range(ANG)]
        total = jnp.dot(
            jnp.concatenate(windows, axis=1),
            tiles[j].reshape(ANG * 256, 128),
            preferred_element_type=F32,
        )
        part[ty, th, tx, rows(c), :] = total.astype(BF)

    def back(c, d):
        def body(i, carry):
            for u in range(2):
                one_tile(c, 2 * i + u, 0, xs[d])
                one_tile(c, ys[d], 1, 2 * i + u)
            return carry

        lax.fori_loop(0, 2, body, 0)

    def remote(src, dst, send, recv, where):
        return pltpu.make_async_remote_copy(
            src_ref=src,
            dst_ref=dst,
            send_sem=send,
            recv_sem=recv,
            device_id=where,
            device_id_type=MESH,
        )

    def first(path, c, d):
        if path == 0:
            src, where = part.at[:, 0, xs[d], rows(c), :], device(xs[d], y, h, s)
        else:
            src, where = part.at[ys[d], 1, :, rows(c), :], device(x, ys[d], h, s)
        return remote(
            src, r1.at[path, c, d - 1], ss1.at[path, c, d - 1], rs1.at[path, c, d - 1], where
        )

    def inner(path, d):
        return device(x, ys[d], h, s) if path == 0 else device(xs[d], y, h, s)

    def outer(path, d):
        return device(xs[d], y, h, s) if path == 0 else device(x, ys[d], h, s)

    def second(path, c, d):
        return remote(
            s2.at[path, c, d - 1],
            r2.at[path, c, d - 1],
            ss2.at[path, c, d - 1],
            rs2.at[path, c, d - 1],
            inner(path, d),
        )

    def across(path, c):
        return remote(
            zs.at[path, c], rz.at[path, c], zss.at[path, c], zrs.at[path, c], device(x, y, 1 - h, s)
        )

    def slot(path, c, k):
        if path == 0:
            return gath.at[ys[(4 - k) % 4], 0, x, :, rows(c)]
        return gath.at[y, 1, xs[(4 - k) % 4], :, rows(c)]

    def gather1(path, c, d):
        ref = slot(path, c, 0)
        return remote(ref, ref, ass1.at[path, c, d - 1], ars1.at[path, c, d - 1], inner(path, d))

    def gather2(path, c, d, k):
        ref = slot(path, c, k)
        return remote(
            ref, ref, ass2.at[path, c, d - 1, k], ars2.at[path, c, d - 1, k], outer(path, d)
        )

    def halo_copy(c, side):
        if side == 0:
            src, where = vt.at[c, 120:128, :], device(x, y, h, sr)
        else:
            src, where = vt.at[c, 0:8, :], device(x, y, h, sl)
        return remote(src, halo.at[c, side], halo_ss.at[c, side], halo_rs.at[c, side], where)

    smooth_copy = remote(smooth, smooth_in, sm_ss, sm_rs, device(x, y, 1 - h, s))

    def send_first(c, d):
        first(0, c, d).start()
        first(1, c, d).start()

    def sum_first(c):
        for path in range(2):
            for d in (1, 2, 3):
                first(path, c, d).wait_recv()
            for d in FAR + (0,):
                at = ys[d] if path == 0 else xs[d]
                own = part[at, 0, x, rows(c), :] if path == 0 else part[y, 1, at, rows(c), :]
                total = own.astype(F32)
                for k in range(3):
                    total = total + r1[path, c, k, at].astype(F32)
                if d:
                    s2[path, c, d - 1] = total.astype(BF)
                    second(path, c, d).start()
                else:
                    keep[path, c] = total

    def sum_second(c):
        for path in range(2):
            for d in (1, 2, 3):
                second(path, c, d).wait_recv()
            total = keep[path, c]
            for k in range(3):
                total = total + r2[path, c, k].astype(F32)
            keep[path, c] = total
            zs[path, c] = total.astype(BF)
            across(path, c).start()

    def finish_volume(c):
        fields = []
        for path in range(2):
            across(path, c).wait_recv()
            base = jnp.where(h == path, smooth[c], smooth_in[c])
            field = base + (keep[path, c] + rz[path, c].astype(F32))
            if c == 1:
                field = jnp.maximum(field, 0.0)
            field = field.T
            fields.append(field)
            gath[y, path, x, :, rows(c)] = field.astype(BF)
            for d in FAR:
                gather1(path, c, d).start()
            for d in FAR:
                gather2(path, c, d, 0).start()
        vnext_ref[:, c, :] = jnp.where(h == 0, fields[0], fields[1])

    def relay(c):
        for k in (1, 3, 2):
            for path in range(2):
                gather1(path, c, k).wait_recv()
                for d in FAR:
                    gather2(path, c, d, k).start()

    def project(c, d, begin, end):
        tx, ty = xs[(4 - d) % 4], ys[(4 - d) % 4]
        if d:
            for path in range(2):
                for k in range(4):
                    gather2(path, c, d, k).wait_recv()
        right = jnp.concatenate(
            [gath[i, 0, tx, :, rows(c)] for i in range(4)]
            + [gath[ty, 1, i, :, rows(c)] for i in range(4)],
            axis=0,
        )
        picks = [i * 8 + tx for i in range(4)] + [ty * 8 + 4 + i for i in range(4)]

        def body(g, carry):
            for u in range(2):
                a = 2 * g + u
                left = jnp.concatenate(
                    [placed_rows(tiles[j, a], band_ref[a, j]) for j in picks], axis=1
                )
                term = jnp.dot(left, right, preferred_element_type=F32)
                if not begin:
                    term = term + acc[c, a]
                if end:
                    out_ref[a, rows(c), :] = term.T
                else:
                    acc[c, a] = term
            return carry

        lax.fori_loop(0, 2, body, 0)

    scale(0)
    band_copy.wait()
    back(0, 2)
    vol_copy.wait()
    for c in range(2):
        vt[c] = vol_ref[:, c, :].T
    pl.semaphore_wait(barrier, len(peers))
    for c in range(2):
        halo_copy(c, 0).start()
        halo_copy(c, 1).start()
    send_first(0, 2)
    back(0, 1)
    send_first(0, 1)
    back(0, 3)
    send_first(0, 3)
    back(0, 0)
    scale(1)
    back(1, 2)
    send_first(1, 2)
    for c in range(2):
        halo_copy(c, 0).wait_recv()
        halo_copy(c, 1).wait_recv()
        mid = vt[c]
        row = lax.broadcasted_iota(jnp.int32, (128, 128), 0)
        low = jnp.where(s > 0, halo[c, 0, 7:8, :], 0.0)
        high = jnp.where(s < SLABS - 1, halo[c, 1, 0:1, :], 0.0)
        before = jnp.where(row == 0, low, pltpu.roll(mid, 1, 0))
        after = jnp.where(row == 127, high, pltpu.roll(mid, 127, 0))
        smooth[c] = mid - SMOOTHING * (2.0 * mid - before - after)
    smooth_copy.start()
    back(1, 1)
    send_first(1, 1)
    back(1, 3)
    sum_first(0)
    send_first(1, 3)
    back(1, 0)
    sum_second(0)
    sum_first(1)
    smooth_copy.wait_recv()
    finish_volume(0)
    sum_second(1)
    relay(0)
    project(0, 0, True, False)
    finish_volume(1)
    relay(1)
    project(0, 1, False, False)
    project(0, 3, False, False)
    project(0, 2, False, True)
    project(1, 0, True, False)
    project(1, 1, False, False)
    project(1, 3, False, False)
    project(1, 2, False, True)

    smooth_copy.wait_send()
    for c in range(2):
        halo_copy(c, 0).wait_send()
        halo_copy(c, 1).wait_send()
        for path in range(2):
            across(path, c).wait_send()
            for d in (1, 2, 3):
                first(path, c, d).wait_send()
                second(path, c, d).wait_send()
                gather1(path, c, d).wait_send()
                for k in range(4):
                    gather2(path, c, d, k).wait_send()


def shards(updates, interp_tiles, band_start, angle_id, angle_weight, volume):
    vmem = pl.BlockSpec(memory_space=pltpu.VMEM)
    hbm = pl.BlockSpec(memory_space=pl.ANY)
    dma = pltpu.SemaphoreType.DMA
    vnext, projection = pl.pallas_call(
        whole_kernel,
        out_shape=(
            jax.ShapeDtypeStruct((128, 2, 128), F32),
            jax.ShapeDtypeStruct((4, 256, 512), F32),
        ),
        in_specs=[hbm] * 6,
        out_specs=(vmem, vmem),
        scratch_shapes=[
            pltpu.SMEM((4, 32), jnp.int32),
            pltpu.SMEM((4,), jnp.int32),
            pltpu.VMEM((1, 128), F32),
            pltpu.VMEM((128, 2, 128), F32),
            pltpu.VMEM((2, 4, 128, 512), F32),
            pltpu.VMEM((32, 4, 256, 128), BF),
            pltpu.VMEM((2, 12, 128, 256), BF),
            pltpu.VMEM((4, 2, 4, 256, 128), BF),
            pltpu.VMEM((2, 128, 128), F32),
            pltpu.VMEM((2, 2, 8, 128), F32),
            pltpu.VMEM((2, 128, 128), F32),
            pltpu.VMEM((2, 128, 128), F32),
            pltpu.VMEM((2, 2, 3, 4, 128, 128), BF),
            pltpu.VMEM((2, 2, 3, 128, 128), BF),
            pltpu.VMEM((2, 2, 3, 128, 128), BF),
            pltpu.VMEM((2, 2, 128, 128), F32),
            pltpu.VMEM((2, 2, 128, 128), BF),
            pltpu.VMEM((2, 2, 128, 128), BF),
            pltpu.VMEM((4, 2, 4, 128, 256), BF),
            pltpu.VMEM((2, 4, 512, 128), F32),
            dma((6,)),
            dma((32,)),
            dma((2, 2)),
            dma((2, 2)),
            dma,
            dma,
            dma((2, 2, 3)),
            dma((2, 2, 3)),
            dma((2, 2, 3)),
            dma((2, 2, 3)),
            dma((2, 2)),
            dma((2, 2)),
            dma((2, 2, 3)),
            dma((2, 2, 3)),
            dma((2, 2, 3, 4)),
            dma((2, 2, 3, 4)),
        ],
        compiler_params=pltpu.CompilerParams(
            collective_id=0, has_side_effects=True, vmem_limit_bytes=63 * 2**20
        ),
        name="exchange",
    )(band_start, angle_id, angle_weight.reshape(1, 128), updates, interp_tiles, volume)
    return vnext, projection.reshape(4, 2, 128, 512)


def solution(mesh):
    placed = (
        P("ang", None, "slab", None),
        P("ang", None, None, None),
        P("ang", None),
        P("ang"),
        P(),
        P("ang", None, "slab"),
    )
    return jax.shard_map(
        shards,
        mesh=mesh,
        in_specs=placed,
        out_specs=(P("ang", None, "slab"), P("ang", None, "slab", None)),
        check_vma=False,
    )
```

```python
import jax
import jax.numpy as jnp
from jax import lax
from jax.experimental import pallas as pl
from jax.experimental.pallas import tpu as pltpu
from jax.sharding import PartitionSpec as P

SMOOTHING = 0.25
MESH = pl.DeviceIdType.MESH
BF = jnp.bfloat16
F32 = jnp.float32
NX, NY, NH = 4, 4, 2
SLABS = 8
ANG = 4
FAR = (2, 1, 3)


def device(x, y, h, s):
    return (y * (NH * NX) + h * NX + x, s)


def wrapped(v, n):
    return lax.rem(v + n, n)


def placed_rows(tile, start):
    low, high = tile[:128], tile[128:]
    zero = jnp.zeros_like(low)
    return jnp.concatenate(
        [
            jnp.where(start == 0, low, zero),
            jnp.where(start == 0, high, jnp.where(start == 1, low, zero)),
            jnp.where(start == 1, high, jnp.where(start == 2, low, zero)),
            jnp.where(start == 2, high, zero),
        ],
        axis=0,
    )


def whole_kernel(
    band_hbm,
    id_hbm,
    weight_hbm,
    upd_hbm,
    tiles_hbm,
    vol_hbm,
    vnext_ref,
    out_hbm,
    band_ref,
    id_ref,
    weight_ref,
    vol_ref,
    upd,
    tiles,
    scaled,
    part,
    vt,
    halo,
    smooth,
    smooth_in,
    r1,
    s2,
    r2,
    keep,
    zs,
    rz,
    gath,
    acc,
    outs,
    out_sem,
    in_sem,
    tile_sem,
    halo_ss,
    halo_rs,
    sm_ss,
    sm_rs,
    ss1,
    rs1,
    ss2,
    rs2,
    zss,
    zrs,
    ass1,
    ars1,
    ass2,
    ars2,
):
    me = lax.axis_index("ang")
    s = lax.axis_index("slab")
    x = lax.rem(me, NX)
    h = lax.rem(me // NX, NH)
    y = me // (NX * NH)
    sl = wrapped(s - 1, SLABS)
    sr = wrapped(s + 1, SLABS)
    xs = [wrapped(x + d, NX) for d in range(4)]
    ys = [wrapped(y + d, NY) for d in range(4)]

    barrier = pltpu.get_barrier_semaphore()
    peers = (
        [device(xs[d], y, h, s) for d in (1, 2, 3)]
        + [device(x, ys[d], h, s) for d in (1, 2, 3)]
        + [device(x, y, 1 - h, s), device(x, y, h, sl), device(x, y, h, sr)]
    )
    for peer in peers:
        pl.semaphore_signal(barrier, inc=1, device_id=peer, device_id_type=MESH)

    def tile_copy(ty, th, tx):
        j = ty * (NH * NX) + th * NX + tx
        return pltpu.make_async_copy(tiles_hbm.at[:, j], tiles.at[j], tile_sem.at[j])

    def start_tiles(d):
        def body(i, carry):
            tile_copy(i, 0, xs[d]).start()
            tile_copy(ys[d], 1, i).start()
            return carry

        lax.fori_loop(0, 4, body, 0)

    band_copy = pltpu.make_async_copy(band_hbm, band_ref, in_sem.at[0])
    id_copy = pltpu.make_async_copy(id_hbm, id_ref, in_sem.at[1])
    weight_copy = pltpu.make_async_copy(weight_hbm, weight_ref, in_sem.at[2])
    vol_copy = pltpu.make_async_copy(vol_hbm, vol_ref, in_sem.at[3])
    upd_copies = [pltpu.make_async_copy(upd_hbm.at[:, c], upd.at[c], in_sem.at[4 + c]) for c in (0, 1)]
    id_copy.start()
    weight_copy.start()
    upd_copies[0].start()
    band_copy.start()
    start_tiles(2)
    vol_copy.start()
    start_tiles(1)
    start_tiles(3)
    upd_copies[1].start()
    start_tiles(0)

    def rows(c):
        return slice(c * 128, c * 128 + 128)

    lanes = lax.broadcasted_iota(jnp.int32, (1, 128), 1)
    id_copy.wait()
    weight_copy.wait()
    chosen = [
        jnp.sum(jnp.where(lanes == id_ref[a], weight_ref[...], 0.0), axis=1, keepdims=True)
        for a in range(ANG)
    ]

    def scale(c):
        upd_copies[c].wait()
        for a in range(ANG):
            value = (chosen[a] * upd[c, a]).astype(BF)
            for k in range(3):
                scaled[c, 3 * a + k] = value[:, 128 * k : 128 * k + 256]

    def one_tile(c, ty, th, tx):
        j = ty * (NH * NX) + th * NX + tx
        windows = [scaled[c, 3 * a + band_ref[a, j]] for a in range(ANG)]
        total = jnp.dot(
            jnp.concatenate(windows, axis=1),
            tiles[j].reshape(ANG * 256, 128),
            preferred_element_type=F32,
        )
        part[ty, th, tx, rows(c), :] = total.astype(BF)

    def back(c, d):
        if c == 0:

            def arrive(i, carry):
                tile_copy(i, 0, xs[d]).wait()
                tile_copy(ys[d], 1, i).wait()
                return carry

            lax.fori_loop(0, 4, arrive, 0)

        def body(i, carry):
            for u in range(2):
                one_tile(c, 2 * i + u, 0, xs[d])
                one_tile(c, ys[d], 1, 2 * i + u)
            return carry

        lax.fori_loop(0, 2, body, 0)

    def remote(src, dst, send, recv, where):
        return pltpu.make_async_remote_copy(
            src_ref=src,
            dst_ref=dst,
            send_sem=send,
            recv_sem=recv,
            device_id=where,
            device_id_type=MESH,
        )

    def first(path, c, d):
        if path == 0:
            src, where = part.at[:, 0, xs[d], rows(c), :], device(xs[d], y, h, s)
        else:
            src, where = part.at[ys[d], 1, :, rows(c), :], device(x, ys[d], h, s)
        return remote(
            src, r1.at[path, c, d - 1], ss1.at[path, c, d - 1], rs1.at[path, c, d - 1], where
        )

    def inner(path, d):
        return device(x, ys[d], h, s) if path == 0 else device(xs[d], y, h, s)

    def outer(path, d):
        return device(xs[d], y, h, s) if path == 0 else device(x, ys[d], h, s)

    def second(path, c, d):
        return remote(
            s2.at[path, c, d - 1],
            r2.at[path, c, d - 1],
            ss2.at[path, c, d - 1],
            rs2.at[path, c, d - 1],
            inner(path, d),
        )

    def across(path, c):
        return remote(
            zs.at[path, c], rz.at[path, c], zss.at[path, c], zrs.at[path, c], device(x, y, 1 - h, s)
        )

    def slot(path, c, k):
        if path == 0:
            return gath.at[ys[(4 - k) % 4], 0, x, :, rows(c)]
        return gath.at[y, 1, xs[(4 - k) % 4], :, rows(c)]

    def gather1(path, c, d):
        ref = slot(path, c, 0)
        return remote(ref, ref, ass1.at[path, c, d - 1], ars1.at[path, c, d - 1], inner(path, d))

    def gather2(path, c, d, k):
        ref = slot(path, c, k)
        return remote(
            ref, ref, ass2.at[path, c, d - 1, k], ars2.at[path, c, d - 1, k], outer(path, d)
        )

    def halo_copy(c, side):
        if side == 0:
            src, where = vt.at[c, 120:128, :], device(x, y, h, sr)
        else:
            src, where = vt.at[c, 0:8, :], device(x, y, h, sl)
        return remote(src, halo.at[c, side], halo_ss.at[c, side], halo_rs.at[c, side], where)

    smooth_copy = remote(smooth, smooth_in, sm_ss, sm_rs, device(x, y, 1 - h, s))

    def send_first(c, d):
        first(0, c, d).start()
        first(1, c, d).start()

    def sum_first(c):
        for path in range(2):
            for d in (1, 2, 3):
                first(path, c, d).wait_recv()
            for d in FAR + (0,):
                at = ys[d] if path == 0 else xs[d]
                own = part[at, 0, x, rows(c), :] if path == 0 else part[y, 1, at, rows(c), :]
                total = own.astype(F32)
                for k in range(3):
                    total = total + r1[path, c, k, at].astype(F32)
                if d:
                    s2[path, c, d - 1] = total.astype(BF)
                    second(path, c, d).start()
                else:
                    keep[path, c] = total

    def sum_second(c):
        for path in range(2):
            for d in (1, 2, 3):
                second(path, c, d).wait_recv()
            total = keep[path, c]
            for k in range(3):
                total = total + r2[path, c, k].astype(F32)
            keep[path, c] = total
            zs[path, c] = total.astype(BF)
            across(path, c).start()

    def finish_volume(c):
        fields = []
        for path in range(2):
            across(path, c).wait_recv()
            base = jnp.where(h == path, smooth[c], smooth_in[c])
            field = base + (keep[path, c] + rz[path, c].astype(F32))
            if c == 1:
                field = jnp.maximum(field, 0.0)
            field = field.T
            fields.append(field)
            gath[y, path, x, :, rows(c)] = field.astype(BF)
            for d in FAR:
                gather1(path, c, d).start()
        for path in range(2):
            for d in FAR:
                gather2(path, c, d, 0).start()
        vnext_ref[:, c, :] = jnp.where(h == 0, fields[0], fields[1])

    def relay(c):
        for k in (1, 3, 2):
            for path in range(2):
                gather1(path, c, k).wait_recv()
                for d in FAR:
                    gather2(path, c, d, k).start()

    def project(c, k, begin, end):
        if k is None:
            places = [(i, 0, x) for i in range(4)] + [(y, 1, i) for i in range(4)]
        else:
            for path in range(2):
                for d in (1, 2, 3):
                    gather2(path, c, d, k).wait_recv()
            places = [(ys[(4 - k) % 4], 0, xs[d]) for d in (1, 2, 3)]
            places += [(ys[d], 1, xs[(4 - k) % 4]) for d in (1, 2, 3)]
        right = jnp.concatenate([gath[ty, th, tx, :, rows(c)] for ty, th, tx in places], axis=0)
        picks = [ty * 8 + th * 4 + tx for ty, th, tx in places]

        def body(g, carry):
            for u in range(2):
                a = 2 * g + u
                left = jnp.concatenate(
                    [placed_rows(tiles[j, a], band_ref[a, j]) for j in picks], axis=1
                )
                term = jnp.dot(left, right, preferred_element_type=F32)
                if not begin:
                    term = term + acc[c, a]
                if end:
                    outs[a, rows(c), :] = term.T
                else:
                    acc[c, a] = term
            return carry

        lax.fori_loop(0, 2, body, 0)
        if end:
            out_copy(c).start()

    def out_copy(c):
        return pltpu.make_async_copy(
            outs.at[:, rows(c), :], out_hbm.at[:, rows(c), :], out_sem.at[c]
        )

    scale(0)
    band_copy.wait()
    back(0, 2)
    vol_copy.wait()
    for c in range(2):
        vt[c] = vol_ref[:, c, :].T
    pl.semaphore_wait(barrier, len(peers))
    send_first(0, 2)
    for c in range(2):
        halo_copy(c, 0).start()
        halo_copy(c, 1).start()
    back(0, 1)
    send_first(0, 1)
    back(0, 3)
    send_first(0, 3)
    scale(1)
    back(1, 2)
    send_first(1, 2)
    back(0, 0)
    for c in range(2):
        halo_copy(c, 0).wait_recv()
        halo_copy(c, 1).wait_recv()
        mid = vt[c]
        row = lax.broadcasted_iota(jnp.int32, (128, 128), 0)
        low = jnp.where(s > 0, halo[c, 0, 7:8, :], 0.0)
        high = jnp.where(s < SLABS - 1, halo[c, 1, 0:1, :], 0.0)
        before = jnp.where(row == 0, low, pltpu.roll(mid, 1, 0))
        after = jnp.where(row == 127, high, pltpu.roll(mid, 127, 0))
        smooth[c] = mid - SMOOTHING * (2.0 * mid - before - after)
    smooth_copy.start()
    back(1, 1)
    back(1, 3)
    back(1, 0)
    sum_first(0)
    send_first(1, 1)
    send_first(1, 3)
    sum_second(0)
    sum_first(1)
    smooth_copy.wait_recv()
    finish_volume(0)
    sum_second(1)
    relay(0)
    project(0, None, True, False)
    project(0, 0, False, False)
    finish_volume(1)
    project(0, 1, False, False)
    project(0, 3, False, False)
    relay(1)
    project(0, 2, False, True)
    project(1, None, True, False)
    project(1, 0, False, False)
    project(1, 1, False, False)
    project(1, 3, False, False)
    project(1, 2, False, True)
    out_copy(0).wait()
    out_copy(1).wait()

    smooth_copy.wait_send()
    for c in range(2):
        halo_copy(c, 0).wait_send()
        halo_copy(c, 1).wait_send()
        for path in range(2):
            across(path, c).wait_send()
            for d in (1, 2, 3):
                first(path, c, d).wait_send()
                second(path, c, d).wait_send()
                gather1(path, c, d).wait_send()
                for k in range(4):
                    gather2(path, c, d, k).wait_send()


def deliver_kernel(small_in, large_in, small_out, large_out, small, large, sems):
    pairs = [(small_in, small, small_out)]
    pairs += [(large_in.at[i], large.at[i], large_out.at[i]) for i in range(large.shape[0])]
    loads = [pltpu.make_async_copy(a, b, sems.at[0, i]) for i, (a, b, c) in enumerate(pairs)]
    stores = [pltpu.make_async_copy(b, c, sems.at[1, i]) for i, (a, b, c) in enumerate(pairs)]
    for load in loads:
        load.start()
    for load, store in zip(loads, stores):
        load.wait()
        store.start()
    for store in stores:
        store.wait()


def shards(updates, interp_tiles, band_start, angle_id, angle_weight, volume):
    vmem = pl.BlockSpec(memory_space=pltpu.VMEM)
    hbm = pl.BlockSpec(memory_space=pl.ANY)
    dma = pltpu.SemaphoreType.DMA
    vnext, projection = pl.pallas_call(
        whole_kernel,
        out_shape=(
            jax.ShapeDtypeStruct((128, 2, 128), F32),
            jax.ShapeDtypeStruct((4, 256, 512), F32),
        ),
        in_specs=[hbm] * 6,
        out_specs=(vmem, hbm),
        scratch_shapes=[
            pltpu.SMEM((4, 32), jnp.int32),
            pltpu.SMEM((4,), jnp.int32),
            pltpu.VMEM((1, 128), F32),
            pltpu.VMEM((128, 2, 128), F32),
            pltpu.VMEM((2, 4, 128, 512), F32),
            pltpu.VMEM((32, 4, 256, 128), BF),
            pltpu.VMEM((2, 12, 128, 256), BF),
            pltpu.VMEM((4, 2, 4, 256, 128), BF),
            pltpu.VMEM((2, 128, 128), F32),
            pltpu.VMEM((2, 2, 8, 128), F32),
            pltpu.VMEM((2, 128, 128), F32),
            pltpu.VMEM((2, 128, 128), F32),
            pltpu.VMEM((2, 2, 3, 4, 128, 128), BF),
            pltpu.VMEM((2, 2, 3, 128, 128), BF),
            pltpu.VMEM((2, 2, 3, 128, 128), BF),
            pltpu.VMEM((2, 2, 128, 128), F32),
            pltpu.VMEM((2, 2, 128, 128), BF),
            pltpu.VMEM((2, 2, 128, 128), BF),
            pltpu.VMEM((4, 2, 4, 128, 256), BF),
            pltpu.VMEM((2, 4, 512, 128), F32),
            pltpu.VMEM((4, 256, 512), F32),
            dma((2,)),
            dma((6,)),
            dma((32,)),
            dma((2, 2)),
            dma((2, 2)),
            dma,
            dma,
            dma((2, 2, 3)),
            dma((2, 2, 3)),
            dma((2, 2, 3)),
            dma((2, 2, 3)),
            dma((2, 2)),
            dma((2, 2)),
            dma((2, 2, 3)),
            dma((2, 2, 3)),
            dma((2, 2, 3, 4)),
            dma((2, 2, 3, 4)),
        ],
        compiler_params=pltpu.CompilerParams(
            collective_id=0, has_side_effects=True, vmem_limit_bytes=63 * 2**20
        ),
        name="exchange",
    )(band_start, angle_id, angle_weight.reshape(1, 128), updates, interp_tiles, volume)
    vnext, projection = pl.pallas_call(
        deliver_kernel,
        out_shape=(
            jax.ShapeDtypeStruct((128, 2, 128), F32),
            jax.ShapeDtypeStruct((8, 128, 512), F32),
        ),
        in_specs=[hbm] * 2,
        out_specs=(hbm, hbm),
        scratch_shapes=[
            pltpu.VMEM((128, 2, 128), F32),
            pltpu.VMEM((8, 128, 512), F32),
            dma((2, 9)),
        ],
        compiler_params=pltpu.CompilerParams(vmem_limit_bytes=63 * 2**20),
        name="deliver",
    )(vnext, projection.reshape(8, 128, 512))
    return vnext, projection.reshape(4, 2, 128, 512)


def solution(mesh):
    placed = (
        P("ang", None, "slab", None),
        P("ang", None, None, None),
        P("ang", None),
        P("ang"),
        P(),
        P("ang", None, "slab"),
    )
    return jax.shard_map(
        shards,
        mesh=mesh,
        in_specs=placed,
        out_specs=(P("ang", None, "slab"), P("ang", None, "slab", None)),
        check_vma=False,
    )
```

```python
import jax
import jax.numpy as jnp
from jax import lax
from jax.experimental import pallas as pl
from jax.experimental.pallas import tpu as pltpu
from jax.sharding import PartitionSpec as P

SMOOTHING = 0.25
MESH = pl.DeviceIdType.MESH
BF = jnp.bfloat16
F32 = jnp.float32
NX, NY, NH = 4, 4, 2
SLABS = 8
ANG = 4
FAR = (2, 1, 3)


def device(x, y, h, s):
    return (y * (NH * NX) + h * NX + x, s)


def wrapped(v, n):
    return lax.rem(v + n, n)


def placed_rows(tile, start):
    low, high = tile[:128], tile[128:]
    zero = jnp.zeros_like(low)
    return jnp.concatenate(
        [
            jnp.where(start == 0, low, zero),
            jnp.where(start == 0, high, jnp.where(start == 1, low, zero)),
            jnp.where(start == 1, high, jnp.where(start == 2, low, zero)),
            jnp.where(start == 2, high, zero),
        ],
        axis=0,
    )


def whole_kernel(
    band_hbm,
    id_hbm,
    weight_hbm,
    upd_hbm,
    tiles_hbm,
    vol_hbm,
    vnext_ref,
    out_hbm,
    band_ref,
    id_ref,
    weight_ref,
    vol_ref,
    upd,
    tiles,
    scaled,
    part,
    vt,
    halo,
    smooth,
    smooth_in,
    rr,
    both,
    r1,
    s2,
    r2,
    keep,
    zs,
    rz,
    gath,
    acc,
    outs,
    out_sem,
    in_sem,
    tile_sem,
    halo_ss,
    halo_rs,
    sm_ss,
    sm_rs,
    trs,
    trr,
    ss2,
    rs2,
    zss,
    zrs,
    ass1,
    ars1,
    ass2,
    ars2,
):
    me = lax.axis_index("ang")
    s = lax.axis_index("slab")
    x = lax.rem(me, NX)
    h = lax.rem(me // NX, NH)
    y = me // (NX * NH)
    sl = wrapped(s - 1, SLABS)
    sr = wrapped(s + 1, SLABS)
    xs = [wrapped(x + d, NX) for d in range(4)]
    ys = [wrapped(y + d, NY) for d in range(4)]

    barrier = pltpu.get_barrier_semaphore()
    peers = (
        [device(xs[d], y, h, s) for d in (1, 2, 3)]
        + [device(x, ys[d], h, s) for d in (1, 2, 3)]
        + [device(x, y, 1 - h, s), device(x, y, h, sl), device(x, y, h, sr)]
    )
    for peer in peers:
        pl.semaphore_signal(barrier, inc=1, device_id=peer, device_id_type=MESH)

    def tile_copy(ty, th, tx):
        j = ty * (NH * NX) + th * NX + tx
        return pltpu.make_async_copy(tiles_hbm.at[:, j], tiles.at[j], tile_sem.at[j])

    def start_tiles(d):
        def body(i, carry):
            tile_copy(i, 0, xs[d]).start()
            tile_copy(ys[d], 1, i).start()
            return carry

        lax.fori_loop(0, 4, body, 0)

    band_copy = pltpu.make_async_copy(band_hbm, band_ref, in_sem.at[0])
    id_copy = pltpu.make_async_copy(id_hbm, id_ref, in_sem.at[1])
    weight_copy = pltpu.make_async_copy(weight_hbm, weight_ref, in_sem.at[2])
    vol_copy = pltpu.make_async_copy(vol_hbm, vol_ref, in_sem.at[3])
    upd_copies = [pltpu.make_async_copy(upd_hbm.at[:, c], upd.at[c], in_sem.at[4 + c]) for c in (0, 1)]
    id_copy.start()
    weight_copy.start()
    upd_copies[0].start()
    band_copy.start()
    start_tiles(2)
    vol_copy.start()
    start_tiles(1)
    start_tiles(3)
    upd_copies[1].start()
    start_tiles(0)

    def rows(c):
        return slice(c * 128, c * 128 + 128)

    lanes = lax.broadcasted_iota(jnp.int32, (1, 128), 1)
    id_copy.wait()
    weight_copy.wait()
    chosen = [
        jnp.sum(jnp.where(lanes == id_ref[a], weight_ref[...], 0.0), axis=1, keepdims=True)
        for a in range(ANG)
    ]

    def scale(c):
        upd_copies[c].wait()
        for a in range(ANG):
            value = (chosen[a] * upd[c, a]).astype(BF)
            for k in range(3):
                scaled[c, 3 * a + k] = value[:, 128 * k : 128 * k + 256]

    def one_tile(c, ty, th, tx):
        j = ty * (NH * NX) + th * NX + tx
        windows = [scaled[c, 3 * a + band_ref[a, j]] for a in range(ANG)]
        total = jnp.dot(
            jnp.concatenate(windows, axis=1),
            tiles[j].reshape(ANG * 256, 128),
            preferred_element_type=F32,
        )
        part[ty, th, tx, rows(c), :] = total.astype(BF)

    def back(c, d):
        if c == 0:

            def arrive(i, carry):
                tile_copy(i, 0, xs[d]).wait()
                tile_copy(ys[d], 1, i).wait()
                return carry

            lax.fori_loop(0, 4, arrive, 0)

        def body(i, carry):
            for u in range(2):
                one_tile(c, 2 * i + u, 0, xs[d])
                one_tile(c, ys[d], 1, 2 * i + u)
            return carry

        lax.fori_loop(0, 2, body, 0)

    def remote(src, dst, send, recv, where):
        return pltpu.make_async_remote_copy(
            src_ref=src,
            dst_ref=dst,
            send_sem=send,
            recv_sem=recv,
            device_id=where,
            device_id_type=MESH,
        )

    def part_of(path, c, d, half):
        two = slice(2 * half, 2 * half + 2)
        if path == 0:
            return part.at[two, 0, xs[d], rows(c), :]
        return part.at[ys[d], 1, two, rows(c), :]

    def step_to(path, side):
        d = 1 if side else 3
        return device(xs[d], y, h, s) if path == 0 else device(x, ys[d], h, s)

    def through(path, c, side):
        return remote(
            part_of(path, c, 2, side),
            rr.at[path, c, side],
            trs.at[0, path, c, side],
            trr.at[0, path, c, side],
            step_to(path, side),
        )

    def direct(path, c, side):
        half = 1 - side
        return remote(
            part_of(path, c, 1 if side else 3, half),
            r1.at[path, c, 0, half],
            trs.at[1, path, c, side],
            trr.at[1, path, c, side],
            step_to(path, side),
        )

    def joined(path, c, side):
        return remote(
            both.at[path, c, side],
            r1.at[path, c, 1, side],
            trs.at[2, path, c, side],
            trr.at[2, path, c, side],
            step_to(path, side),
        )

    def join(c):
        for path in range(2):
            for side in range(2):
                through(path, c, side).wait_recv()
                own = part_of(path, c, 1 if side else 3, side)[...].astype(F32)
                both[path, c, side] = (own + rr[path, c, side].astype(F32)).astype(BF)
                joined(path, c, side).start()

    def send_through(c):
        for side in range(2):
            for path in range(2):
                through(path, c, side).start()

    def send_direct(c, side):
        for path in range(2):
            direct(path, c, side).start()

    def inner(path, d):
        return device(x, ys[d], h, s) if path == 0 else device(xs[d], y, h, s)

    def outer(path, d):
        return device(xs[d], y, h, s) if path == 0 else device(x, ys[d], h, s)

    def second(path, c, d):
        return remote(
            s2.at[path, c, d - 1],
            r2.at[path, c, d - 1],
            ss2.at[path, c, d - 1],
            rs2.at[path, c, d - 1],
            inner(path, d),
        )

    def across(path, c):
        return remote(
            zs.at[path, c], rz.at[path, c], zss.at[path, c], zrs.at[path, c], device(x, y, 1 - h, s)
        )

    def slot(path, c, k):
        if path == 0:
            return gath.at[ys[(4 - k) % 4], 0, x, :, rows(c)]
        return gath.at[y, 1, xs[(4 - k) % 4], :, rows(c)]

    def gather1(path, c, d):
        ref = slot(path, c, 0)
        return remote(ref, ref, ass1.at[path, c, d - 1], ars1.at[path, c, d - 1], inner(path, d))

    def gather2(path, c, d, k):
        ref = slot(path, c, k)
        return remote(
            ref, ref, ass2.at[path, c, d - 1, k], ars2.at[path, c, d - 1, k], outer(path, d)
        )

    def halo_copy(c, side):
        if side == 0:
            src, where = vt.at[c, 120:128, :], device(x, y, h, sr)
        else:
            src, where = vt.at[c, 0:8, :], device(x, y, h, sl)
        return remote(src, halo.at[c, side], halo_ss.at[c, side], halo_rs.at[c, side], where)

    smooth_copy = remote(smooth, smooth_in, sm_ss, sm_rs, device(x, y, 1 - h, s))

    def sum_first(c):
        for path in range(2):
            for side in range(2):
                direct(path, c, side).wait_recv()
                joined(path, c, side).wait_recv()
            for d in FAR + (0,):
                at = ys[d] if path == 0 else xs[d]
                own = part[at, 0, x, rows(c), :] if path == 0 else part[y, 1, at, rows(c), :]
                total = own.astype(F32)
                for k in range(2):
                    total = total + r1[path, c, k, at // 2, lax.rem(at, 2)].astype(F32)
                if d:
                    s2[path, c, d - 1] = total.astype(BF)
                    second(path, c, d).start()
                else:
                    keep[path, c] = total

    def sum_second(c):
        for path in range(2):
            for d in (1, 2, 3):
                second(path, c, d).wait_recv()
            total = keep[path, c]
            for k in range(3):
                total = total + r2[path, c, k].astype(F32)
            keep[path, c] = total
            zs[path, c] = total.astype(BF)
            across(path, c).start()

    def finish_volume(c):
        fields = []
        for path in range(2):
            across(path, c).wait_recv()
            base = jnp.where(h == path, smooth[c], smooth_in[c])
            field = base + (keep[path, c] + rz[path, c].astype(F32))
            if c == 1:
                field = jnp.maximum(field, 0.0)
            field = field.T
            fields.append(field)
            gath[y, path, x, :, rows(c)] = field.astype(BF)
            for d in FAR:
                gather1(path, c, d).start()
        vnext_ref[:, c, :] = jnp.where(h == 0, fields[0], fields[1])

    def spread(path, c, k):
        for d in FAR:
            gather2(path, c, d, k).start()

    def send_own(c):
        for path in range(2):
            spread(path, c, 0)

    def relay(c, order=(1, 3, 2)):
        for k in order:
            for path in range(2):
                gather1(path, c, k).wait_recv()
                spread(path, c, k)

    def project(channels, k, begin, end):
        if k is None:
            places = [(i, 0, x) for i in range(4)] + [(y, 1, i) for i in range(4)]
        else:
            for path in range(2):
                for c in channels:
                    for d in FAR:
                        gather2(path, c, d, k).wait_recv()
            places = [(ys[(4 - k) % 4], 0, xs[d]) for d in (1, 2, 3)]
            places += [(ys[d], 1, xs[(4 - k) % 4]) for d in (1, 2, 3)]
        cols = slice(channels[0] * 128, channels[-1] * 128 + 128)
        right = jnp.concatenate([gath[ty, th, tx, :, cols] for ty, th, tx in places], axis=0)
        picks = [ty * 8 + th * 4 + tx for ty, th, tx in places]
        for a in range(ANG):
            left = jnp.concatenate(
                [placed_rows(tiles[j, a], band_ref[a, j]) for j in picks], axis=1
            )
            term = jnp.dot(left, right, preferred_element_type=F32)
            if not begin:
                term = term + acc[a, :, cols]
            if end:
                outs[a, cols, :] = term.T
                out_copy(a).start()
            else:
                acc[a, :, cols] = term

    def out_copy(a):
        return pltpu.make_async_copy(outs.at[a], out_hbm.at[a], out_sem.at[a])

    scale(0)
    band_copy.wait()
    back(0, 2)
    vol_copy.wait()
    for c in range(2):
        vt[c] = vol_ref[:, c, :].T
    pl.semaphore_wait(barrier, len(peers))
    send_through(0)
    for c in range(2):
        halo_copy(c, 0).start()
        halo_copy(c, 1).start()
    back(0, 1)
    send_direct(0, 1)
    back(0, 3)
    send_direct(0, 0)
    scale(1)
    back(1, 2)
    send_through(1)
    back(0, 0)
    for c in range(2):
        halo_copy(c, 0).wait_recv()
        halo_copy(c, 1).wait_recv()
        mid = vt[c]
        row = lax.broadcasted_iota(jnp.int32, (128, 128), 0)
        low = jnp.where(s > 0, halo[c, 0, 7:8, :], 0.0)
        high = jnp.where(s < SLABS - 1, halo[c, 1, 0:1, :], 0.0)
        before = jnp.where(row == 0, low, pltpu.roll(mid, 1, 0))
        after = jnp.where(row == 127, high, pltpu.roll(mid, 127, 0))
        smooth[c] = mid - SMOOTHING * (2.0 * mid - before - after)
    smooth_copy.start()
    join(0)
    back(1, 1)
    send_direct(1, 1)
    back(1, 3)
    send_direct(1, 0)
    back(1, 0)
    join(1)
    sum_first(0)
    sum_first(1)
    sum_second(0)
    sum_second(1)
    smooth_copy.wait_recv()
    finish_volume(0)
    send_own(0)
    finish_volume(1)
    relay(0)
    send_own(1)
    project((0,), None, True, False)
    relay(1)
    project((1,), None, True, False)
    project((0,), 0, False, False)
    project((1,), 0, False, False)
    project((0, 1), 1, False, False)
    project((0, 1), 3, False, False)
    project((0, 1), 2, False, True)
    for a in range(ANG):
        out_copy(a).wait()

    smooth_copy.wait_send()
    for c in range(2):
        halo_copy(c, 0).wait_send()
        halo_copy(c, 1).wait_send()
        for path in range(2):
            across(path, c).wait_send()
            for side in range(2):
                through(path, c, side).wait_send()
                direct(path, c, side).wait_send()
                joined(path, c, side).wait_send()
            for d in (1, 2, 3):
                second(path, c, d).wait_send()
                gather1(path, c, d).wait_send()
            for k in range(4):
                for d in FAR:
                    gather2(path, c, d, k).wait_send()


def deliver_kernel(small_in, large_in, small_out, large_out, small, large, sems):
    pairs = [(small_in, small, small_out)]
    pairs += [(large_in.at[i], large.at[i], large_out.at[i]) for i in range(large.shape[0])]
    loads = [pltpu.make_async_copy(a, b, sems.at[0, i]) for i, (a, b, c) in enumerate(pairs)]
    stores = [pltpu.make_async_copy(b, c, sems.at[1, i]) for i, (a, b, c) in enumerate(pairs)]
    for load in loads:
        load.start()
    for load, store in zip(loads, stores):
        load.wait()
        store.start()
    for store in stores:
        store.wait()


def shards(updates, interp_tiles, band_start, angle_id, angle_weight, volume):
    vmem = pl.BlockSpec(memory_space=pltpu.VMEM)
    hbm = pl.BlockSpec(memory_space=pl.ANY)
    dma = pltpu.SemaphoreType.DMA
    vnext, projection = pl.pallas_call(
        whole_kernel,
        out_shape=(
            jax.ShapeDtypeStruct((128, 2, 128), F32),
            jax.ShapeDtypeStruct((4, 256, 512), F32),
        ),
        in_specs=[hbm] * 6,
        out_specs=(vmem, hbm),
        scratch_shapes=[
            pltpu.SMEM((4, 32), jnp.int32),
            pltpu.SMEM((4,), jnp.int32),
            pltpu.VMEM((1, 128), F32),
            pltpu.VMEM((128, 2, 128), F32),
            pltpu.VMEM((2, 4, 128, 512), F32),
            pltpu.VMEM((32, 4, 256, 128), BF),
            pltpu.VMEM((2, 12, 128, 256), BF),
            pltpu.VMEM((4, 2, 4, 256, 128), BF),
            pltpu.VMEM((2, 128, 128), F32),
            pltpu.VMEM((2, 2, 8, 128), F32),
            pltpu.VMEM((2, 128, 128), F32),
            pltpu.VMEM((2, 128, 128), F32),
            pltpu.VMEM((2, 2, 2, 2, 128, 128), BF),
            pltpu.VMEM((2, 2, 2, 2, 128, 128), BF),
            pltpu.VMEM((2, 2, 2, 2, 2, 128, 128), BF),
            pltpu.VMEM((2, 2, 3, 128, 128), BF),
            pltpu.VMEM((2, 2, 3, 128, 128), BF),
            pltpu.VMEM((2, 2, 128, 128), F32),
            pltpu.VMEM((2, 2, 128, 128), BF),
            pltpu.VMEM((2, 2, 128, 128), BF),
            pltpu.VMEM((4, 2, 4, 128, 256), BF),
            pltpu.VMEM((4, 512, 256), F32),
            pltpu.VMEM((4, 256, 512), F32),
            dma((4,)),
            dma((6,)),
            dma((32,)),
            dma((2, 2)),
            dma((2, 2)),
            dma,
            dma,
            dma((3, 2, 2, 2)),
            dma((3, 2, 2, 2)),
            dma((2, 2, 3)),
            dma((2, 2, 3)),
            dma((2, 2)),
            dma((2, 2)),
            dma((2, 2, 3)),
            dma((2, 2, 3)),
            dma((2, 2, 3, 4)),
            dma((2, 2, 3, 4)),
        ],
        compiler_params=pltpu.CompilerParams(
            collective_id=0, has_side_effects=True, vmem_limit_bytes=63 * 2**20
        ),
        name="exchange",
    )(band_start, angle_id, angle_weight.reshape(1, 128), updates, interp_tiles, volume)
    vnext, projection = pl.pallas_call(
        deliver_kernel,
        out_shape=(
            jax.ShapeDtypeStruct((128, 2, 128), F32),
            jax.ShapeDtypeStruct((8, 128, 512), F32),
        ),
        in_specs=[hbm] * 2,
        out_specs=(hbm, hbm),
        scratch_shapes=[
            pltpu.VMEM((128, 2, 128), F32),
            pltpu.VMEM((8, 128, 512), F32),
            dma((2, 9)),
        ],
        compiler_params=pltpu.CompilerParams(vmem_limit_bytes=63 * 2**20),
        name="deliver",
    )(vnext, projection.reshape(8, 128, 512))
    return vnext, projection.reshape(4, 2, 128, 512)


def solution(mesh):
    placed = (
        P("ang", None, "slab", None),
        P("ang", None, None, None),
        P("ang", None),
        P("ang"),
        P(),
        P("ang", None, "slab"),
    )
    return jax.shard_map(
        shards,
        mesh=mesh,
        in_specs=placed,
        out_specs=(P("ang", None, "slab"), P("ang", None, "slab", None)),
        check_vma=False,
    )
```

```python
import jax
import jax.numpy as jnp
from jax import lax
from jax.experimental import pallas as pl
from jax.experimental.pallas import tpu as pltpu
from jax.sharding import PartitionSpec as P

SMOOTHING = 0.25
MESH = pl.DeviceIdType.MESH
BF = jnp.bfloat16
F32 = jnp.float32
NX, NY, NH = 4, 4, 2
SLABS = 8
ANG = 4
FAR = (2, 1, 3)


def device(x, y, h, s):
    return (y * (NH * NX) + h * NX + x, s)


def wrapped(v, n):
    return lax.rem(v + n, n)


def placed_rows(tile, start):
    low, high = tile[:128], tile[128:]
    zero = jnp.zeros_like(low)
    return jnp.concatenate(
        [
            jnp.where(start == 0, low, zero),
            jnp.where(start == 0, high, jnp.where(start == 1, low, zero)),
            jnp.where(start == 1, high, jnp.where(start == 2, low, zero)),
            jnp.where(start == 2, high, zero),
        ],
        axis=0,
    )


def whole_kernel(
    band_hbm,
    id_hbm,
    weight_hbm,
    upd_hbm,
    tiles_hbm,
    vol_hbm,
    vnext_ref,
    out_hbm,
    band_ref,
    id_ref,
    weight_ref,
    vol_ref,
    upd,
    tiles,
    scaled,
    part,
    vt,
    halo,
    smooth,
    smooth_in,
    rr,
    both,
    r1,
    s2,
    r2,
    keep,
    zs,
    rz,
    gath,
    acc,
    outs,
    out_sem,
    in_sem,
    tile_sem,
    halo_ss,
    halo_rs,
    sm_ss,
    sm_rs,
    trs,
    trr,
    ss2,
    rs2,
    zss,
    zrs,
    ass1,
    ars1,
    ass2,
    ars2,
):
    me = lax.axis_index("ang")
    s = lax.axis_index("slab")
    x = lax.rem(me, NX)
    h = lax.rem(me // NX, NH)
    y = me // (NX * NH)
    sl = wrapped(s - 1, SLABS)
    sr = wrapped(s + 1, SLABS)
    xs = [wrapped(x + d, NX) for d in range(4)]
    ys = [wrapped(y + d, NY) for d in range(4)]

    barrier = pltpu.get_barrier_semaphore()
    peers = (
        [device(xs[d], y, h, s) for d in (1, 2, 3)]
        + [device(x, ys[d], h, s) for d in (1, 2, 3)]
        + [device(x, y, 1 - h, s), device(x, y, h, sl), device(x, y, h, sr)]
    )
    for peer in peers:
        pl.semaphore_signal(barrier, inc=1, device_id=peer, device_id_type=MESH)

    def tile_copy(ty, th, tx):
        j = ty * (NH * NX) + th * NX + tx
        return pltpu.make_async_copy(tiles_hbm.at[:, j], tiles.at[j], tile_sem.at[j])

    def start_tiles(d):
        def body(i, carry):
            tile_copy(i, 0, xs[d]).start()
            tile_copy(ys[d], 1, i).start()
            return carry

        lax.fori_loop(0, 4, body, 0)

    band_copy = pltpu.make_async_copy(band_hbm, band_ref, in_sem.at[0])
    id_copy = pltpu.make_async_copy(id_hbm, id_ref, in_sem.at[1])
    weight_copy = pltpu.make_async_copy(weight_hbm, weight_ref, in_sem.at[2])
    vol_copy = pltpu.make_async_copy(vol_hbm, vol_ref, in_sem.at[3])
    upd_copies = [pltpu.make_async_copy(upd_hbm.at[:, c], upd.at[c], in_sem.at[4 + c]) for c in (0, 1)]
    id_copy.start()
    weight_copy.start()
    upd_copies[0].start()
    band_copy.start()
    start_tiles(2)
    vol_copy.start()
    start_tiles(1)
    start_tiles(3)
    upd_copies[1].start()
    start_tiles(0)

    def rows(c):
        return slice(c * 128, c * 128 + 128)

    lanes = lax.broadcasted_iota(jnp.int32, (1, 128), 1)
    id_copy.wait()
    weight_copy.wait()
    chosen = [
        jnp.sum(jnp.where(lanes == id_ref[a], weight_ref[...], 0.0), axis=1, keepdims=True)
        for a in range(ANG)
    ]

    def scale(c):
        upd_copies[c].wait()
        for a in range(ANG):
            value = (chosen[a] * upd[c, a]).astype(BF)
            for k in range(3):
                scaled[c, 3 * a + k] = value[:, 128 * k : 128 * k + 256]

    def one_tile(c, ty, th, tx):
        j = ty * (NH * NX) + th * NX + tx
        windows = [scaled[c, 3 * a + band_ref[a, j]] for a in range(ANG)]
        total = jnp.dot(
            jnp.concatenate(windows, axis=1),
            tiles[j].reshape(ANG * 256, 128),
            preferred_element_type=F32,
        )
        part[ty, th, tx, rows(c), :] = total.astype(BF)

    def back(c, d, begin=0, end=2):
        if c == 0:

            def arrive(i, carry):
                tile_copy(i, 0, xs[d]).wait()
                tile_copy(ys[d], 1, i).wait()
                return carry

            lax.fori_loop(2 * begin, 2 * end, arrive, 0)

        def body(i, carry):
            for u in range(2):
                one_tile(c, 2 * i + u, 0, xs[d])
                one_tile(c, ys[d], 1, 2 * i + u)
            return carry

        lax.fori_loop(begin, end, body, 0)

    def remote(src, dst, send, recv, where):
        return pltpu.make_async_remote_copy(
            src_ref=src,
            dst_ref=dst,
            send_sem=send,
            recv_sem=recv,
            device_id=where,
            device_id_type=MESH,
        )

    def part_of(path, c, d, half):
        two = slice(2 * half, 2 * half + 2)
        if path == 0:
            return part.at[two, 0, xs[d], rows(c), :]
        return part.at[ys[d], 1, two, rows(c), :]

    def step_to(path, side):
        d = 1 if side else 3
        return device(xs[d], y, h, s) if path == 0 else device(x, ys[d], h, s)

    def through(path, c, side):
        return remote(
            part_of(path, c, 2, side),
            rr.at[path, c, side],
            trs.at[0, path, c, side],
            trr.at[0, path, c, side],
            step_to(path, side),
        )

    def direct(path, c, side):
        half = 1 - side
        return remote(
            part_of(path, c, 1 if side else 3, half),
            r1.at[path, c, 0, half],
            trs.at[1, path, c, side],
            trr.at[1, path, c, side],
            step_to(path, side),
        )

    def joined(path, c, side):
        return remote(
            both.at[path, c, side],
            r1.at[path, c, 1, side],
            trs.at[2, path, c, side],
            trr.at[2, path, c, side],
            step_to(path, side),
        )

    def join(c):
        for path in range(2):
            for side in range(2):
                through(path, c, side).wait_recv()
                own = part_of(path, c, 1 if side else 3, side)[...].astype(F32)
                both[path, c, side] = (own + rr[path, c, side].astype(F32)).astype(BF)
                joined(path, c, side).start()

    def send_through(c, side):
        for path in range(2):
            through(path, c, side).start()

    def send_direct(c, side):
        for path in range(2):
            direct(path, c, side).start()

    def inner(path, d):
        return device(x, ys[d], h, s) if path == 0 else device(xs[d], y, h, s)

    def outer(path, d):
        return device(xs[d], y, h, s) if path == 0 else device(x, ys[d], h, s)

    def second(path, c, d):
        return remote(
            s2.at[path, c, d - 1],
            r2.at[path, c, d - 1],
            ss2.at[path, c, d - 1],
            rs2.at[path, c, d - 1],
            inner(path, d),
        )

    def across(path, c):
        return remote(
            zs.at[path, c], rz.at[path, c], zss.at[path, c], zrs.at[path, c], device(x, y, 1 - h, s)
        )

    def slot(path, c, k):
        if path == 0:
            return gath.at[ys[(4 - k) % 4], 0, x, :, rows(c)]
        return gath.at[y, 1, xs[(4 - k) % 4], :, rows(c)]

    def gather1(path, c, d):
        ref = slot(path, c, 0)
        return remote(ref, ref, ass1.at[path, c, d - 1], ars1.at[path, c, d - 1], inner(path, d))

    def gather2(path, c, d, k):
        ref = slot(path, c, k)
        return remote(
            ref, ref, ass2.at[path, c, d - 1, k], ars2.at[path, c, d - 1, k], outer(path, d)
        )

    def halo_copy(c, side):
        if side == 0:
            src, where = vt.at[c, 120:128, :], device(x, y, h, sr)
        else:
            src, where = vt.at[c, 0:8, :], device(x, y, h, sl)
        return remote(src, halo.at[c, side], halo_ss.at[c, side], halo_rs.at[c, side], where)

    smooth_copy = remote(smooth, smooth_in, sm_ss, sm_rs, device(x, y, 1 - h, s))

    def sum_first(c):
        for path in range(2):
            for side in range(2):
                direct(path, c, side).wait_recv()
                joined(path, c, side).wait_recv()
            for d in FAR + (0,):
                at = ys[d] if path == 0 else xs[d]
                own = part[at, 0, x, rows(c), :] if path == 0 else part[y, 1, at, rows(c), :]
                total = own.astype(F32)
                for k in range(2):
                    total = total + r1[path, c, k, at // 2, lax.rem(at, 2)].astype(F32)
                if d:
                    s2[path, c, d - 1] = total.astype(BF)
                    second(path, c, d).start()
                else:
                    keep[path, c] = total

    def sum_second(c):
        for path in range(2):
            for d in (1, 2, 3):
                second(path, c, d).wait_recv()
            total = keep[path, c]
            for k in range(3):
                total = total + r2[path, c, k].astype(F32)
            keep[path, c] = total
            zs[path, c] = total.astype(BF)
            across(path, c).start()

    def finish_volume(c):
        fields = []
        for path in range(2):
            across(path, c).wait_recv()
            base = jnp.where(h == path, smooth[c], smooth_in[c])
            field = base + (keep[path, c] + rz[path, c].astype(F32))
            if c == 1:
                field = jnp.maximum(field, 0.0)
            field = field.T
            fields.append(field)
            gath[y, path, x, :, rows(c)] = field.astype(BF)
            for d in FAR:
                gather1(path, c, d).start()
        vnext_ref[:, c, :] = jnp.where(h == 0, fields[0], fields[1])

    def spread(path, c, k):
        for d in FAR:
            gather2(path, c, d, k).start()

    def send_own(c):
        for path in range(2):
            spread(path, c, 0)

    def relay(c, order=(1, 3, 2)):
        for k in order:
            for path in range(2):
                gather1(path, c, k).wait_recv()
                spread(path, c, k)

    def project(channels, k, begin, end):
        if k is None:
            places = [(i, 0, x) for i in range(4)] + [(y, 1, i) for i in range(4)]
        else:
            for path in range(2):
                for c in channels:
                    for d in FAR:
                        gather2(path, c, d, k).wait_recv()
            places = [(ys[(4 - k) % 4], 0, xs[d]) for d in (1, 2, 3)]
            places += [(ys[d], 1, xs[(4 - k) % 4]) for d in (1, 2, 3)]
        cols = slice(channels[0] * 128, channels[-1] * 128 + 128)
        right = jnp.concatenate([gath[ty, th, tx, :, cols] for ty, th, tx in places], axis=0)
        picks = [ty * 8 + th * 4 + tx for ty, th, tx in places]
        for a in range(ANG):
            left = jnp.concatenate(
                [placed_rows(tiles[j, a], band_ref[a, j]) for j in picks], axis=1
            )
            term = jnp.dot(left, right, preferred_element_type=F32)
            if not begin:
                term = term + acc[a, :, cols]
            if end:
                outs[a, cols, :] = term.T
                out_copy(a).start()
            else:
                acc[a, :, cols] = term

    def out_copy(a):
        return pltpu.make_async_copy(outs.at[a], out_hbm.at[a], out_sem.at[a])

    scale(0)
    band_copy.wait()
    back(0, 2, 0, 1)
    pl.semaphore_wait(barrier, len(peers))
    send_through(0, 0)
    back(0, 2, 1, 2)
    send_through(0, 1)
    vol_copy.wait()
    for c in range(2):
        vt[c] = vol_ref[:, c, :].T
    for c in range(2):
        halo_copy(c, 0).start()
        halo_copy(c, 1).start()
    back(0, 1)
    send_direct(0, 1)
    back(0, 3)
    send_direct(0, 0)
    scale(1)
    back(1, 2)
    send_through(1, 0)
    send_through(1, 1)
    back(0, 0)
    for c in range(2):
        halo_copy(c, 0).wait_recv()
        halo_copy(c, 1).wait_recv()
        mid = vt[c]
        row = lax.broadcasted_iota(jnp.int32, (128, 128), 0)
        low = jnp.where(s > 0, halo[c, 0, 7:8, :], 0.0)
        high = jnp.where(s < SLABS - 1, halo[c, 1, 0:1, :], 0.0)
        before = jnp.where(row == 0, low, pltpu.roll(mid, 1, 0))
        after = jnp.where(row == 127, high, pltpu.roll(mid, 127, 0))
        smooth[c] = mid - SMOOTHING * (2.0 * mid - before - after)
    smooth_copy.start()
    join(0)
    back(1, 1)
    send_direct(1, 1)
    back(1, 3)
    send_direct(1, 0)
    back(1, 0)
    join(1)
    sum_first(0)
    sum_first(1)
    sum_second(0)
    sum_second(1)
    smooth_copy.wait_recv()
    finish_volume(0)
    send_own(0)
    finish_volume(1)
    relay(0)
    send_own(1)
    project((0,), None, True, False)
    relay(1)
    project((1,), None, True, False)
    project((0,), 0, False, False)
    project((1,), 0, False, False)
    project((0, 1), 1, False, False)
    project((0, 1), 3, False, False)
    project((0, 1), 2, False, True)
    for a in range(ANG):
        out_copy(a).wait()

    smooth_copy.wait_send()
    for c in range(2):
        halo_copy(c, 0).wait_send()
        halo_copy(c, 1).wait_send()
        for path in range(2):
            across(path, c).wait_send()
            for side in range(2):
                through(path, c, side).wait_send()
                direct(path, c, side).wait_send()
                joined(path, c, side).wait_send()
            for d in (1, 2, 3):
                second(path, c, d).wait_send()
                gather1(path, c, d).wait_send()
            for k in range(4):
                for d in FAR:
                    gather2(path, c, d, k).wait_send()


def deliver_kernel(small_in, large_in, small_out, large_out, small, large, sems):
    pairs = [(small_in, small, small_out)]
    pairs += [(large_in.at[i], large.at[i], large_out.at[i]) for i in range(large.shape[0])]
    loads = [pltpu.make_async_copy(a, b, sems.at[0, i]) for i, (a, b, c) in enumerate(pairs)]
    stores = [pltpu.make_async_copy(b, c, sems.at[1, i]) for i, (a, b, c) in enumerate(pairs)]
    for load in loads:
        load.start()
    for load, store in zip(loads, stores):
        load.wait()
        store.start()
    for store in stores:
        store.wait()


def shards(updates, interp_tiles, band_start, angle_id, angle_weight, volume):
    vmem = pl.BlockSpec(memory_space=pltpu.VMEM)
    hbm = pl.BlockSpec(memory_space=pl.ANY)
    dma = pltpu.SemaphoreType.DMA
    vnext, projection = pl.pallas_call(
        whole_kernel,
        out_shape=(
            jax.ShapeDtypeStruct((128, 2, 128), F32),
            jax.ShapeDtypeStruct((4, 256, 512), F32),
        ),
        in_specs=[hbm] * 6,
        out_specs=(vmem, hbm),
        scratch_shapes=[
            pltpu.SMEM((4, 32), jnp.int32),
            pltpu.SMEM((4,), jnp.int32),
            pltpu.VMEM((1, 128), F32),
            pltpu.VMEM((128, 2, 128), F32),
            pltpu.VMEM((2, 4, 128, 512), F32),
            pltpu.VMEM((32, 4, 256, 128), BF),
            pltpu.VMEM((2, 12, 128, 256), BF),
            pltpu.VMEM((4, 2, 4, 256, 128), BF),
            pltpu.VMEM((2, 128, 128), F32),
            pltpu.VMEM((2, 2, 8, 128), F32),
            pltpu.VMEM((2, 128, 128), F32),
            pltpu.VMEM((2, 128, 128), F32),
            pltpu.VMEM((2, 2, 2, 2, 128, 128), BF),
            pltpu.VMEM((2, 2, 2, 2, 128, 128), BF),
            pltpu.VMEM((2, 2, 2, 2, 2, 128, 128), BF),
            pltpu.VMEM((2, 2, 3, 128, 128), BF),
            pltpu.VMEM((2, 2, 3, 128, 128), BF),
            pltpu.VMEM((2, 2, 128, 128), F32),
            pltpu.VMEM((2, 2, 128, 128), BF),
            pltpu.VMEM((2, 2, 128, 128), BF),
            pltpu.VMEM((4, 2, 4, 128, 256), BF),
            pltpu.VMEM((4, 512, 256), F32),
            pltpu.VMEM((4, 256, 512), F32),
            dma((4,)),
            dma((6,)),
            dma((32,)),
            dma((2, 2)),
            dma((2, 2)),
            dma,
            dma,
            dma((3, 2, 2, 2)),
            dma((3, 2, 2, 2)),
            dma((2, 2, 3)),
            dma((2, 2, 3)),
            dma((2, 2)),
            dma((2, 2)),
            dma((2, 2, 3)),
            dma((2, 2, 3)),
            dma((2, 2, 3, 4)),
            dma((2, 2, 3, 4)),
        ],
        compiler_params=pltpu.CompilerParams(
            collective_id=0, has_side_effects=True, vmem_limit_bytes=63 * 2**20
        ),
        name="exchange",
    )(band_start, angle_id, angle_weight.reshape(1, 128), updates, interp_tiles, volume)
    vnext, projection = pl.pallas_call(
        deliver_kernel,
        out_shape=(
            jax.ShapeDtypeStruct((128, 2, 128), F32),
            jax.ShapeDtypeStruct((8, 128, 512), F32),
        ),
        in_specs=[hbm] * 2,
        out_specs=(hbm, hbm),
        scratch_shapes=[
            pltpu.VMEM((128, 2, 128), F32),
            pltpu.VMEM((8, 128, 512), F32),
            dma((2, 9)),
        ],
        compiler_params=pltpu.CompilerParams(vmem_limit_bytes=63 * 2**20),
        name="deliver",
    )(vnext, projection.reshape(8, 128, 512))
    return vnext, projection.reshape(4, 2, 128, 512)


def solution(mesh):
    placed = (
        P("ang", None, "slab", None),
        P("ang", None, None, None),
        P("ang", None),
        P("ang"),
        P(),
        P("ang", None, "slab"),
    )
    return jax.shard_map(
        shards,
        mesh=mesh,
        in_specs=placed,
        out_specs=(P("ang", None, "slab"), P("ang", None, "slab", None)),
        check_vma=False,
    )
```

```python
import jax
import jax.numpy as jnp
from jax import lax
from jax.experimental import pallas as pl
from jax.experimental.pallas import tpu as pltpu
from jax.sharding import PartitionSpec as P

SMOOTHING = 0.25
MESH = pl.DeviceIdType.MESH
BF = jnp.bfloat16
F32 = jnp.float32
NX, NY, NH = 4, 4, 2
SLABS = 8
ANG = 4
FAR = (2, 1, 3)


def device(x, y, h, s):
    return (y * (NH * NX) + h * NX + x, s)


def wrapped(v, n):
    return lax.rem(v + n, n)


def placed_rows(tile, start):
    low, high = tile[:128], tile[128:]
    zero = jnp.zeros_like(low)
    return jnp.concatenate(
        [
            jnp.where(start == 0, low, zero),
            jnp.where(start == 0, high, jnp.where(start == 1, low, zero)),
            jnp.where(start == 1, high, jnp.where(start == 2, low, zero)),
            jnp.where(start == 2, high, zero),
        ],
        axis=0,
    )


def whole_kernel(
    band_hbm,
    id_hbm,
    weight_hbm,
    upd_hbm,
    tiles_hbm,
    vol_hbm,
    vnext_ref,
    out_hbm,
    band_ref,
    id_ref,
    weight_ref,
    vol_ref,
    upd,
    tiles,
    scaled,
    part,
    vt,
    halo,
    smooth,
    smooth_in,
    rr,
    both,
    r1,
    s2,
    r2,
    keep,
    zs,
    rz,
    gath,
    acc,
    outs,
    out_sem,
    in_sem,
    tile_sem,
    halo_ss,
    halo_rs,
    sm_ss,
    sm_rs,
    trs,
    trr,
    ss2,
    rs2,
    zss,
    zrs,
    ass1,
    ars1,
    ass2,
    ars2,
):
    me = lax.axis_index("ang")
    s = lax.axis_index("slab")
    x = lax.rem(me, NX)
    h = lax.rem(me // NX, NH)
    y = me // (NX * NH)
    sl = wrapped(s - 1, SLABS)
    sr = wrapped(s + 1, SLABS)
    xs = [wrapped(x + d, NX) for d in range(4)]
    ys = [wrapped(y + d, NY) for d in range(4)]

    barrier = pltpu.get_barrier_semaphore()
    peers = (
        [device(xs[d], y, h, s) for d in (1, 2, 3)]
        + [device(x, ys[d], h, s) for d in (1, 2, 3)]
        + [device(x, y, 1 - h, s), device(x, y, h, sl), device(x, y, h, sr)]
    )
    for peer in peers:
        pl.semaphore_signal(barrier, inc=1, device_id=peer, device_id_type=MESH)

    def tile_copy(ty, th, tx):
        j = ty * (NH * NX) + th * NX + tx
        return pltpu.make_async_copy(tiles_hbm.at[:, j], tiles.at[j], tile_sem.at[j])

    def start_tiles(d):
        def body(i, carry):
            tile_copy(i, 0, xs[d]).start()
            tile_copy(ys[d], 1, i).start()
            return carry

        lax.fori_loop(0, 4, body, 0)

    band_copy = pltpu.make_async_copy(band_hbm, band_ref, in_sem.at[0])
    id_copy = pltpu.make_async_copy(id_hbm, id_ref, in_sem.at[1])
    weight_copy = pltpu.make_async_copy(weight_hbm, weight_ref, in_sem.at[2])
    vol_copy = pltpu.make_async_copy(vol_hbm, vol_ref, in_sem.at[3])
    upd_copies = [pltpu.make_async_copy(upd_hbm.at[:, c], upd.at[c], in_sem.at[4 + c]) for c in (0, 1)]
    id_copy.start()
    weight_copy.start()
    upd_copies[0].start()
    band_copy.start()
    start_tiles(2)
    vol_copy.start()
    start_tiles(1)
    start_tiles(3)
    upd_copies[1].start()
    start_tiles(0)

    def rows(c):
        return slice(c * 128, c * 128 + 128)

    lanes = lax.broadcasted_iota(jnp.int32, (1, 128), 1)
    id_copy.wait()
    weight_copy.wait()
    chosen = [
        jnp.sum(jnp.where(lanes == id_ref[a], weight_ref[...], 0.0), axis=1, keepdims=True)
        for a in range(ANG)
    ]

    def scale(c):
        upd_copies[c].wait()
        for a in range(ANG):
            value = (chosen[a] * upd[c, a]).astype(BF)
            for k in range(3):
                scaled[c, 3 * a + k] = value[:, 128 * k : 128 * k + 256]

    def one_tile(c, ty, th, tx):
        j = ty * (NH * NX) + th * NX + tx
        windows = [scaled[c, 3 * a + band_ref[a, j]] for a in range(ANG)]
        total = jnp.dot(
            jnp.concatenate(windows, axis=1),
            tiles[j].reshape(ANG * 256, 128),
            preferred_element_type=F32,
        )
        part[ty, th, tx, rows(c), :] = total.astype(BF)

    def back(c, d, begin=0, end=2):
        if c == 0:

            def arrive(i, carry):
                tile_copy(i, 0, xs[d]).wait()
                tile_copy(ys[d], 1, i).wait()
                return carry

            lax.fori_loop(2 * begin, 2 * end, arrive, 0)

        def body(i, carry):
            for u in range(2):
                one_tile(c, 2 * i + u, 0, xs[d])
                one_tile(c, ys[d], 1, 2 * i + u)
            return carry

        lax.fori_loop(begin, end, body, 0)

    def remote(src, dst, send, recv, where):
        return pltpu.make_async_remote_copy(
            src_ref=src,
            dst_ref=dst,
            send_sem=send,
            recv_sem=recv,
            device_id=where,
            device_id_type=MESH,
        )

    def part_of(path, c, d, half):
        two = slice(2 * half, 2 * half + 2)
        if path == 0:
            return part.at[two, 0, xs[d], rows(c), :]
        return part.at[ys[d], 1, two, rows(c), :]

    def step_to(path, side):
        d = 1 if side else 3
        return device(xs[d], y, h, s) if path == 0 else device(x, ys[d], h, s)

    def through(path, c, side):
        return remote(
            part_of(path, c, 2, side),
            rr.at[path, c, side],
            trs.at[0, path, c, side],
            trr.at[0, path, c, side],
            step_to(path, side),
        )

    def direct(path, c, side):
        half = 1 - side
        return remote(
            part_of(path, c, 1 if side else 3, half),
            r1.at[path, c, 0, half],
            trs.at[1, path, c, side],
            trr.at[1, path, c, side],
            step_to(path, side),
        )

    def joined(path, c, side):
        return remote(
            both.at[path, c, side],
            r1.at[path, c, 1, side],
            trs.at[2, path, c, side],
            trr.at[2, path, c, side],
            step_to(path, side),
        )

    def join(c):
        for path in range(2):
            for side in range(2):
                through(path, c, side).wait_recv()
                own = part_of(path, c, 1 if side else 3, side)[...].astype(F32)
                both[path, c, side] = (own + rr[path, c, side].astype(F32)).astype(BF)
                joined(path, c, side).start()

    def send_through(c, side):
        for path in range(2):
            through(path, c, side).start()

    def send_direct(c, side):
        for path in range(2):
            direct(path, c, side).start()

    def inner(path, d):
        return device(x, ys[d], h, s) if path == 0 else device(xs[d], y, h, s)

    def outer(path, d):
        return device(xs[d], y, h, s) if path == 0 else device(x, ys[d], h, s)

    def second(path, c, d):
        return remote(
            s2.at[path, c, d - 1],
            r2.at[path, c, d - 1],
            ss2.at[path, c, d - 1],
            rs2.at[path, c, d - 1],
            inner(path, d),
        )

    def across(path, c):
        return remote(
            zs.at[path, c], rz.at[path, c], zss.at[path, c], zrs.at[path, c], device(x, y, 1 - h, s)
        )

    def slot(path, c, k):
        if path == 0:
            return gath.at[ys[(4 - k) % 4], 0, x, :, rows(c)]
        return gath.at[y, 1, xs[(4 - k) % 4], :, rows(c)]

    def gather1(path, c, d):
        ref = slot(path, c, 0)
        return remote(ref, ref, ass1.at[path, c, d - 1], ars1.at[path, c, d - 1], inner(path, d))

    def gather2(path, c, d, k):
        ref = slot(path, c, k)
        return remote(
            ref, ref, ass2.at[path, c, d - 1, k], ars2.at[path, c, d - 1, k], outer(path, d)
        )

    def halo_copy(c, side):
        if side == 0:
            src, where = vt.at[c, 120:128, :], device(x, y, h, sr)
        else:
            src, where = vt.at[c, 0:8, :], device(x, y, h, sl)
        return remote(src, halo.at[c, side], halo_ss.at[c, side], halo_rs.at[c, side], where)

    smooth_copy = remote(smooth, smooth_in, sm_ss, sm_rs, device(x, y, 1 - h, s))

    def sum_first(c):
        for path in range(2):
            for side in range(2):
                direct(path, c, side).wait_recv()
                joined(path, c, side).wait_recv()
            for d in FAR + (0,):
                at = ys[d] if path == 0 else xs[d]
                own = part[at, 0, x, rows(c), :] if path == 0 else part[y, 1, at, rows(c), :]
                total = own.astype(F32)
                for k in range(2):
                    total = total + r1[path, c, k, at // 2, lax.rem(at, 2)].astype(F32)
                if d:
                    s2[path, c, d - 1] = total.astype(BF)
                    second(path, c, d).start()
                else:
                    keep[path, c] = total

    def sum_second(c):
        for path in range(2):
            for d in (1, 2, 3):
                second(path, c, d).wait_recv()
            total = keep[path, c]
            for k in range(3):
                total = total + r2[path, c, k].astype(F32)
            keep[path, c] = total
            zs[path, c] = total.astype(BF)
            across(path, c).start()

    def finish_volume(c):
        fields = []
        for path in range(2):
            across(path, c).wait_recv()
            base = jnp.where(h == path, smooth[c], smooth_in[c])
            field = base + (keep[path, c] + rz[path, c].astype(F32))
            if c == 1:
                field = jnp.maximum(field, 0.0)
            field = field.T
            fields.append(field)
            gath[y, path, x, :, rows(c)] = field.astype(BF)
            for d in FAR:
                gather1(path, c, d).start()
        smooth[c] = jnp.where(h == 0, fields[0], fields[1])

    def spread(path, c, k):
        for d in FAR:
            gather2(path, c, d, k).start()

    def send_own(c):
        for path in range(2):
            spread(path, c, 0)

    def relay(c, order=(1, 3, 2)):
        for k in order:
            for path in range(2):
                gather1(path, c, k).wait_recv()
                spread(path, c, k)

    def project(channels, k, begin, end):
        if k is None:
            places = [(i, 0, x) for i in range(4)] + [(y, 1, i) for i in range(4)]
        else:
            for path in range(2):
                for c in channels:
                    for d in FAR:
                        gather2(path, c, d, k).wait_recv()
            places = [(ys[(4 - k) % 4], 0, xs[d]) for d in (1, 2, 3)]
            places += [(ys[d], 1, xs[(4 - k) % 4]) for d in (1, 2, 3)]
        cols = slice(channels[0] * 128, channels[-1] * 128 + 128)
        right = jnp.concatenate([gath[ty, th, tx, :, cols] for ty, th, tx in places], axis=0)
        picks = [ty * 8 + th * 4 + tx for ty, th, tx in places]
        for a in range(ANG):
            left = jnp.concatenate(
                [placed_rows(tiles[j, a], band_ref[a, j]) for j in picks], axis=1
            )
            term = jnp.dot(left, right, preferred_element_type=F32)
            if not begin:
                term = term + acc[a, :, cols]
            if end:
                outs[a, cols, :] = term.T
                out_copy(a).start()
            else:
                acc[a, :, cols] = term

    def out_copy(a):
        return pltpu.make_async_copy(outs.at[a], out_hbm.at[a], out_sem.at[a])

    scale(0)
    band_copy.wait()
    back(0, 2, 0, 1)
    pl.semaphore_wait(barrier, len(peers))
    send_through(0, 0)
    back(0, 2, 1, 2)
    send_through(0, 1)
    vol_copy.wait()
    for c in range(2):
        vt[c] = vol_ref[:, c, :].T
    for c in range(2):
        halo_copy(c, 0).start()
        halo_copy(c, 1).start()
    back(0, 1)
    send_direct(0, 1)
    back(0, 3)
    send_direct(0, 0)
    scale(1)
    back(1, 2)
    send_through(1, 0)
    send_through(1, 1)
    back(0, 0)
    for c in range(2):
        halo_copy(c, 0).wait_recv()
        halo_copy(c, 1).wait_recv()
        mid = vt[c]
        row = lax.broadcasted_iota(jnp.int32, (128, 128), 0)
        low = jnp.where(s > 0, halo[c, 0, 7:8, :], 0.0)
        high = jnp.where(s < SLABS - 1, halo[c, 1, 0:1, :], 0.0)
        before = jnp.where(row == 0, low, pltpu.roll(mid, 1, 0))
        after = jnp.where(row == 127, high, pltpu.roll(mid, 127, 0))
        smooth[c] = mid - SMOOTHING * (2.0 * mid - before - after)
    smooth_copy.start()
    join(0)
    back(1, 1)
    send_direct(1, 1)
    back(1, 3)
    send_direct(1, 0)
    back(1, 0)
    join(1)
    sum_first(0)
    sum_first(1)
    sum_second(0)
    sum_second(1)
    smooth_copy.wait()
    finish_volume(0)
    send_own(0)
    finish_volume(1)
    send_own(1)
    relay(0)
    project((0,), None, True, False)
    relay(1)
    for c in range(2):
        vnext_ref[:, c, :] = smooth[c]
    project((1,), None, True, False)
    project((0,), 0, False, False)
    project((1,), 0, False, False)
    project((0, 1), 1, False, False)
    project((0, 1), 3, False, False)
    project((0, 1), 2, False, True)
    for a in range(ANG):
        out_copy(a).wait()

    for c in range(2):
        halo_copy(c, 0).wait_send()
        halo_copy(c, 1).wait_send()
        for path in range(2):
            across(path, c).wait_send()
            for side in range(2):
                through(path, c, side).wait_send()
                direct(path, c, side).wait_send()
                joined(path, c, side).wait_send()
            for d in (1, 2, 3):
                second(path, c, d).wait_send()
                gather1(path, c, d).wait_send()
            for k in range(4):
                for d in FAR:
                    gather2(path, c, d, k).wait_send()


def deliver_kernel(small_in, large_in, small_out, large_out, small, large, sems):
    pairs = [(small_in, small, small_out)]
    pairs += [(large_in.at[i], large.at[i], large_out.at[i]) for i in range(large.shape[0])]
    loads = [pltpu.make_async_copy(a, b, sems.at[0, i]) for i, (a, b, c) in enumerate(pairs)]
    stores = [pltpu.make_async_copy(b, c, sems.at[1, i]) for i, (a, b, c) in enumerate(pairs)]
    for load in loads:
        load.start()
    for load, store in zip(loads, stores):
        load.wait()
        store.start()
    for store in stores:
        store.wait()


def shards(updates, interp_tiles, band_start, angle_id, angle_weight, volume):
    vmem = pl.BlockSpec(memory_space=pltpu.VMEM)
    hbm = pl.BlockSpec(memory_space=pl.ANY)
    dma = pltpu.SemaphoreType.DMA
    vnext, projection = pl.pallas_call(
        whole_kernel,
        out_shape=(
            jax.ShapeDtypeStruct((128, 2, 128), F32),
            jax.ShapeDtypeStruct((4, 256, 512), F32),
        ),
        in_specs=[hbm] * 6,
        out_specs=(vmem, hbm),
        scratch_shapes=[
            pltpu.SMEM((4, 32), jnp.int32),
            pltpu.SMEM((4,), jnp.int32),
            pltpu.VMEM((1, 128), F32),
            pltpu.VMEM((128, 2, 128), F32),
            pltpu.VMEM((2, 4, 128, 512), F32),
            pltpu.VMEM((32, 4, 256, 128), BF),
            pltpu.VMEM((2, 12, 128, 256), BF),
            pltpu.VMEM((4, 2, 4, 256, 128), BF),
            pltpu.VMEM((2, 128, 128), F32),
            pltpu.VMEM((2, 2, 8, 128), F32),
            pltpu.VMEM((2, 128, 128), F32),
            pltpu.VMEM((2, 128, 128), F32),
            pltpu.VMEM((2, 2, 2, 2, 128, 128), BF),
            pltpu.VMEM((2, 2, 2, 2, 128, 128), BF),
            pltpu.VMEM((2, 2, 2, 2, 2, 128, 128), BF),
            pltpu.VMEM((2, 2, 3, 128, 128), BF),
            pltpu.VMEM((2, 2, 3, 128, 128), BF),
            pltpu.VMEM((2, 2, 128, 128), F32),
            pltpu.VMEM((2, 2, 128, 128), BF),
            pltpu.VMEM((2, 2, 128, 128), BF),
            pltpu.VMEM((4, 2, 4, 128, 256), BF),
            pltpu.VMEM((4, 512, 256), F32),
            pltpu.VMEM((4, 256, 512), F32),
            dma((4,)),
            dma((6,)),
            dma((32,)),
            dma((2, 2)),
            dma((2, 2)),
            dma,
            dma,
            dma((3, 2, 2, 2)),
            dma((3, 2, 2, 2)),
            dma((2, 2, 3)),
            dma((2, 2, 3)),
            dma((2, 2)),
            dma((2, 2)),
            dma((2, 2, 3)),
            dma((2, 2, 3)),
            dma((2, 2, 3, 4)),
            dma((2, 2, 3, 4)),
        ],
        compiler_params=pltpu.CompilerParams(
            collective_id=0, has_side_effects=True, vmem_limit_bytes=63 * 2**20
        ),
        name="exchange",
    )(band_start, angle_id, angle_weight.reshape(1, 128), updates, interp_tiles, volume)
    vnext, projection = pl.pallas_call(
        deliver_kernel,
        out_shape=(
            jax.ShapeDtypeStruct((128, 2, 128), F32),
            jax.ShapeDtypeStruct((8, 128, 512), F32),
        ),
        in_specs=[hbm] * 2,
        out_specs=(hbm, hbm),
        scratch_shapes=[
            pltpu.VMEM((128, 2, 128), F32),
            pltpu.VMEM((8, 128, 512), F32),
            dma((2, 9)),
        ],
        compiler_params=pltpu.CompilerParams(vmem_limit_bytes=63 * 2**20),
        name="deliver",
    )(vnext, projection.reshape(8, 128, 512))
    return vnext, projection.reshape(4, 2, 128, 512)


def solution(mesh):
    placed = (
        P("ang", None, "slab", None),
        P("ang", None, None, None),
        P("ang", None),
        P("ang"),
        P(),
        P("ang", None, "slab"),
    )
    return jax.shard_map(
        shards,
        mesh=mesh,
        in_specs=placed,
        out_specs=(P("ang", None, "slab"), P("ang", None, "slab", None)),
        check_vma=False,
    )
```
